32 devices in a mesh: seq: 16 (over z, x, core), chan: 2 (over y).
Axes of the slice: x: 2, y: 2, z: 4, core: 2. Of those that a mesh axis runs over, the one named last changes fastest.
Arguments:
- gate_input: bfloat16 [1024, 4096], P('seq', 'chan'), may hold values from -6 to 6
- key_input: bfloat16 [1024, 4096], P('seq', 'chan'), may hold values from -6 to 6
- value_input: bfloat16 [1024, 4096], P('seq', 'chan'), may hold values from -6 to 6
- decay_rate: float32 [16, 4096], P(None, 'chan'), may hold values from 0.0009765625 to 0.1
- residue: float32 [16, 4096], P(None, 'chan'), may hold values from -1.5 to 1.5
- skip_gain: float32 [4096], P('chan'), may hold values from -3 to 3
- out_weight: bfloat16 [4096, 4096], P('chan', 'seq'), may hold values from -0.125 to 0.125
Outputs:
- mixed: bfloat16 [1024, 4096], P('seq', 'chan')
The draws below stay inside these ranges and needn't reach their ends.
All inputs are finite; a program needn't handle non-finite values.
Results may differ from the reference program's by a relative error of at most 0.014.
Values may be sent and summed in bfloat16 or wider, within the bound.
A program may use at most 64 MiB of HBM per device.

```python
import math
import jax
import jax.numpy as jnp
from jax import lax

D = 4096
MODES = 16
TOK_DEV = 64
LENGTH = 1024
N_SEQ = 16
N_CHAN = 2


def strengthened(array, own_key, source, target, blocks, factor):
    owner, partner = [(jnp.arange(array.shape[dim]) // (array.shape[dim] // blocks)).reshape([-1 if axis == dim else 1 for axis in range(array.ndim)]) for dim in (source, target)]
    chosen = jax.random.permutation(own_key, blocks)[partner]
    strong = (owner == chosen) | (owner == (partner + blocks // 2) % blocks)
    return jnp.where(strong, factor * array, array)


def block_scale(rng, extent, split, smallest, top_value):
    loudness, own = 1.0, jax.random.fold_in(rng, 6)
    for dim, shards_of in split:
        steps = jnp.exp(jax.random.uniform(jax.random.fold_in(own, dim), (shards_of,), jnp.float32, smallest / len(split), top_value / len(split)))
        loudness = loudness * jnp.repeat(steps, extent[dim] // shards_of).reshape([-1 if axis == dim else 1 for axis in range(len(extent))])
    return loudness


def gaussian(rng, dims, width, most, shards=(), dtype=jnp.bfloat16):
    drawn = width * jax.random.normal(rng, dims, jnp.float32)
    if shards:
        drawn = drawn * block_scale(rng, dims, shards, -0.22, 0.18)
    return jnp.clip(drawn, -most, most).astype(dtype)


def gaussian_with(stream_key, dims, scale, reach, cuts, heavy, dtype=jnp.bfloat16):
    values = scale * jax.random.normal(stream_key, dims, jnp.float32)
    if cuts:
        values = values * block_scale(stream_key, dims, cuts, -0.22, 0.18)
    return jnp.clip(strengthened(values, jax.random.fold_in(stream_key, 3), *heavy), -reach, reach).astype(dtype)


def setup_inputs(seed: int = 0) -> dict:
    splits = jax.random.split(jax.random.key(seed), 8)
    return {
        "gate_input": gaussian(splits[0], (LENGTH, D), 1.0, 6.0, ((0, 16), (1, 2))),
        "key_input": gaussian(splits[1], (LENGTH, D), 1.0, 6.0, ((0, 16), (1, 2))),
        "value_input": gaussian(splits[2], (LENGTH, D), 1.0, 6.0, ((0, 16), (1, 2))),
        "decay_rate": jnp.clip(jnp.exp(math.log(0.1) - 4.6288867 * jax.random.uniform(splits[3], (MODES, D), jnp.float32) ** block_scale(splits[3], (MODES, D), ((1, 2),), -0.2, 0.2)), 0.0009765625, 0.1),
        "residue": gaussian(splits[4], (MODES, D), MODES ** -0.5, 1.5, ((1, 2),), jnp.float32),
        "skip_gain": gaussian(splits[5], (D,), 0.5, 3.0, ((0, 2),), jnp.float32),
        "out_weight": gaussian_with(splits[6], (D, D), D ** -0.5, 0.125, ((0, 2), (1, 16)), (0, 1, 16, 2.0)),
    }


def reference(gate_input, key_input, value_input, decay_rate, residue, skip_gain, out_weight):
    total_rows = TOK_DEV * N_SEQ
    padded_len = 2 * total_rows
    group_cols = D // N_CHAN
    signal = key_input.astype(jnp.float32) * value_input.astype(jnp.float32)
    amplitude = residue * jnp.sqrt(-jnp.expm1(-2.0 * decay_rate))
    positions = jnp.arange(total_rows).astype(jnp.float32)
    pieces = []
    for group_index in range(N_CHAN):
        first_col = group_index * group_cols
        group_signal = signal[:, first_col:first_col + group_cols]
        rates = decay_rate[:, first_col:first_col + group_cols]
        amps = amplitude[:, first_col:first_col + group_cols]

        def add_mode(mode_index, totals):
            return totals + amps[mode_index][None, :] * jnp.exp(-rates[mode_index][None, :] * positions[:, None])
        response = lax.fori_loop(0, MODES, add_mode, jnp.zeros((total_rows, group_cols), jnp.float32))
        product = jnp.fft.rfft(group_signal, n=padded_len, axis=0) * jnp.fft.rfft(response, n=padded_len, axis=0)
        pieces.append(jnp.fft.irfft(product, n=padded_len, axis=0)[:total_rows])
    convolved = jnp.concatenate(pieces, axis=1)
    gated_rows = (gate_input.astype(jnp.float32) * (convolved + skip_gain[None, :] * signal)).astype(jnp.bfloat16)
    summed = jnp.zeros((total_rows, D), jnp.float32)
    for group_index in range(N_CHAN):
        first_col = group_index * group_cols
        partial_sum = jnp.dot(gated_rows[:, first_col:first_col + group_cols].astype(jnp.float32), out_weight[first_col:first_col + group_cols].astype(jnp.float32), precision=lax.Precision.HIGHEST)
        summed = summed + partial_sum.astype(jnp.bfloat16).astype(jnp.float32)
    return summed.astype(jnp.bfloat16)
```

```python
import functools

import jax
import jax.numpy as jnp
from jax import lax
from jax.experimental import pallas as pl
from jax.experimental.pallas import tpu as pltpu
from jax.sharding import PartitionSpec as P

MESH = pl.DeviceIdType.MESH
F32 = jnp.float32
BF16 = jnp.bfloat16
LANES = 128
SUB = 8
SLAB = 4
HALVES = 2
PIECES = 2


def one_minus_exp(y):
    series = jnp.ones_like(y)
    for order in range(10, 1, -1):
        series = 1.0 - y * (1.0 / order) * series
    return jnp.where(y < 0.4, y * series, 1.0 - jnp.exp(-y))


def column_parts(width):
    return 2 if width % (2 * LANES) == 0 else 1


def kernel(
    n, n_chan,
    q_hbm, k_hbm, v_hbm, rate_hbm, residue_hbm, skip_hbm, w_hbm, out_hbm,
    q_ref, k_ref, v_ref, rate_ref, amp_ref, skip_ref, w_ref, w_other, load_sem, w_send, w_recv,
    sig, local, padded, ends, ends_all, carry_in, carry_out, starts_all, starts,
    gathered, partial, arrived, summed, landed, out_ref,
    ready, end_send, end_recv, carry_send, carry_recv, start_send, start_recv,
    line_send, line_recv, sib_send, sib_recv, cross_send, cross_recv, part_send, part_recv,
):
    loads = [
        pltpu.make_async_copy(source, target, load_sem.at[i])
        for i, (source, target) in enumerate([
            (k_hbm, k_ref), (v_hbm, v_ref), (rate_hbm, rate_ref),
            (residue_hbm, amp_ref), (skip_hbm, skip_ref), (q_hbm, q_ref), (w_hbm, w_ref),
        ])
    ]
    for load in loads:
        load.start()
    tok, chans = q_ref.shape
    modes = rate_ref.shape[0]
    blocks = chans // LANES
    width = w_ref.shape[1]
    per_chan = n // n_chan
    line = n // SLAB
    tiles = tok // SUB
    quarter_blocks = blocks // SLAB
    quarter = quarter_blocks * modes
    half = tok // HALVES
    parts = column_parts(width)
    cols = width // parts
    direct = width % LANES == 0

    me = lax.axis_index("seq")
    chan = lax.axis_index("chan")
    z = me // SLAB
    x = (me // 2) % 2
    c = me % 2
    qd = me % SLAB
    sib = me + 1 - 2 * c
    across = me + 2 - 4 * x
    has_right = z < line - 1
    has_left = z > 0
    out_chan = me // per_chan
    owner_plane = chan == out_chan

    def mate(turn):
        return me - qd + lax.rem(qd + turn, SLAB)

    barrier = pltpu.get_barrier_semaphore()

    def hello(seq, ch):
        pl.semaphore_signal(barrier, inc=1, device_id=(seq, ch), device_id_type=MESH)

    for turn in range(1, SLAB):
        hello(mate(turn), chan)
    pl.when(has_right)(lambda: hello(me + SLAB, chan))
    pl.when(has_left)(lambda: hello(me - SLAB, chan))
    for turn in range(1, n_chan):
        hello(me, lax.rem(chan + turn, n_chan))
    greeters = SLAB - 1 + n_chan - 1 + has_right.astype(jnp.int32) + has_left.astype(jnp.int32)
    steps = lax.broadcasted_iota(jnp.int32, (SUB, LANES), 0).astype(F32)

    def lanes(b):
        return pl.ds(pl.multiple_of(b * LANES, LANES), LANES)

    for load in loads[:3]:
        load.wait()

    def end_block(b, _):
        at = lanes(b)
        s = k_ref[:, at].astype(F32) * v_ref[:, at].astype(F32)
        sig[:, at] = s
        found = []
        for m in range(modes):
            rate = rate_ref[pl.ds(m, 1), at]
            jump = jnp.exp(-float(SUB) * rate)
            total = s[:SUB]
            for t in range(1, tiles):
                total = total * jump + s[t * SUB:(t + 1) * SUB]
            total = total * jnp.exp(-rate * (float(SUB - 1) - steps))
            found.append(jnp.sum(total, axis=0, keepdims=True))
        ends[pl.ds(pl.multiple_of(b * modes, modes), modes)] = jnp.concatenate(found, axis=0).astype(BF16)
        return 0

    lax.fori_loop(0, blocks, end_block, 0)

    pl.semaphore_wait(barrier, greeters)

    def quarter_rows(p):
        return pl.ds(pl.multiple_of(p * quarter, quarter), quarter)

    def slab_copy(source, target, send_sem, recv_sem, turn):
        return pltpu.make_async_remote_copy(
            src_ref=source, dst_ref=target, send_sem=send_sem, recv_sem=recv_sem,
            device_id=(mate(turn), chan), device_id_type=MESH,
        )

    def slab_wait(ref, sem):
        return slab_copy(ref, ref, sem, sem, 1)

    for turn in (2, 3, 1):
        slab_copy(ends.at[quarter_rows(lax.rem(qd + turn, SLAB))], ends_all.at[qd], end_send, end_recv, turn).start()
    ends_all[qd] = ends[quarter_rows(qd)]

    def swap(part, first, rows):
        at = (pl.ds(first, rows), pl.ds(part * cols, cols))
        pltpu.make_async_remote_copy(
            src_ref=w_hbm.at[at], dst_ref=w_other.at[at],
            send_sem=w_send.at[part], recv_sem=w_recv.at[part],
            device_id=(across, chan), device_id_type=MESH,
        ).start()

    def swapped(part):
        at = (slice(None), pl.ds(part * cols, cols))
        return pltpu.make_async_remote_copy(
            src_ref=w_other.at[at], dst_ref=w_other.at[at],
            send_sem=w_send.at[part], recv_sem=w_recv.at[part],
            device_id=(across, chan), device_id_type=MESH,
        )

    block_rows = LANES // 4
    middle_rows = chans * 7 // 32

    loads[3].wait()
    loads[4].wait()
    amp_ref[...] = amp_ref[...] * jnp.sqrt(one_minus_exp(2.0 * rate_ref[...]))

    padded[:SUB] = jnp.zeros((SUB, LANES), F32)

    def local_block(b, _):
        swap(0, pl.multiple_of(b * block_rows, block_rows), block_rows)
        at = lanes(b)
        response = [jnp.zeros((SUB, LANES), F32)] * tiles
        for m in range(modes):
            rate = rate_ref[pl.ds(m, 1), at]
            jump = jnp.exp(-float(SUB) * rate)
            term = amp_ref[pl.ds(m, 1), at] * jnp.exp(-rate * steps)
            for t in range(tiles):
                response[t] = response[t] + term
                if t < tiles - 1:
                    term = term * jump
        padded[SUB:] = jnp.concatenate(response, axis=0)
        skip = skip_ref[:, at]
        totals = [skip * sig[t * SUB:(t + 1) * SUB, at] for t in range(tiles)]
        for lag in range(SUB):
            moved = [padded[pl.ds(SUB - lag + t * SUB, SUB)] for t in range(tiles)]
            for first in range(tiles):
                value = sig[pl.ds(first * SUB + lag, 1), at]
                for t in range(first, tiles):
                    totals[t] = totals[t] + moved[t - first] * value
        for t in range(tiles):
            local[t * SUB:(t + 1) * SUB, at] = totals[t]
        return 0

    lax.fori_loop(0, blocks, local_block, 0)

    def signal_left():
        pl.semaphore_signal(ready, inc=1, device_id=(me - SLAB, chan), device_id_type=MESH)

    pl.when(z < line - 2)(lambda: pl.semaphore_wait(ready, 1))
    pl.when(jnp.logical_and(has_left, has_right))(signal_left)

    fades = jnp.concatenate(
        [jnp.exp(-float(tok) * rate_ref[:, lanes(qd * quarter_blocks + j)]) for j in range(quarter_blocks)], axis=0
    )
    slab_wait(ends_all.at[pl.ds(0, SLAB - 1)], end_recv).wait_recv()
    found = [ends_all[p].astype(F32) for p in range(SLAB)]
    slab_total = found[0]
    for p in range(1, SLAB):
        slab_total = slab_total * fades + found[p]
    slab_fade = (fades * fades) * (fades * fades)

    def carry_copy(hop):
        return pltpu.make_async_remote_copy(
            src_ref=carry_out, dst_ref=carry_in.at[z], send_sem=carry_send.at[hop - 1], recv_sem=carry_recv.at[z],
            device_id=(me + hop * SLAB, chan), device_id_type=MESH,
        )

    @pl.when(has_right)
    def _():
        carry_out[...] = slab_total.astype(BF16)
        for hop in range(1, line):
            pl.when(z + hop < line)(carry_copy(hop).start)

    @pl.when(has_left)
    def _():
        swap(0, blocks * block_rows, middle_rows)

    def collect(i, carry):
        pltpu.make_async_remote_copy(
            src_ref=carry_in.at[i], dst_ref=carry_in.at[i], send_sem=carry_send.at[0], recv_sem=carry_recv.at[i],
            device_id=(sib, chan), device_id_type=MESH,
        ).wait_recv()
        return carry * slab_fade + carry_in[i].astype(F32)

    carry = lax.fori_loop(0, z, collect, jnp.zeros((quarter, LANES), F32))

    state = carry
    for p in range(SLAB):
        starts_all[p] = state.astype(BF16)
        if p < SLAB - 1:
            state = state * fades + found[p]
    for turn in (2, 3, 1):
        slab_copy(
            starts_all.at[lax.rem(qd + turn, SLAB)], starts.at[quarter_rows(qd)], start_send, start_recv, turn
        ).start()
    starts[quarter_rows(qd)] = starts_all[qd]

    @pl.when(jnp.logical_not(has_left))
    def _():
        swap(0, blocks * block_rows, middle_rows)

    swap(0, blocks * block_rows + middle_rows, chans - blocks * block_rows - middle_rows)
    for part in range(1, parts):
        swap(part, 0, chans)
    loads[5].wait()
    slab_wait(starts.at[pl.ds(0, (SLAB - 1) * quarter)], start_recv).wait_recv()

    half_tiles = tiles // HALVES
    own_rows = [pl.multiple_of(((z * HALVES + h) * 2 + c) * half, half) for h in range(HALVES)]

    def gate_half(h):
        def gate_block(b, _):
            at = lanes(b)
            held = starts[pl.ds(pl.multiple_of(b * modes, modes), modes)].astype(F32)
            totals = [
                local[(h * half_tiles + t) * SUB:(h * half_tiles + t + 1) * SUB, at] for t in range(half_tiles)
            ]
            for m in range(modes):
                rate = rate_ref[pl.ds(m, 1), at]
                jump = jnp.exp(-float(SUB) * rate)
                term = (amp_ref[pl.ds(m, 1), at] * held[m:m + 1]) * jnp.exp(-rate * (steps + float(1 + h * half)))
                for t in range(half_tiles):
                    totals[t] = totals[t] + term
                    if t < half_tiles - 1:
                        term = term * jump
            q = q_ref[h * half:(h + 1) * half, at].astype(F32)
            gathered[pl.ds(own_rows[h], half), at] = (q * jnp.concatenate(totals, axis=0)).astype(BF16)
            return 0

        lax.fori_loop(0, blocks, gate_block, 0)

    piece_rows = half // PIECES

    def line_copy(h, p, zz, peer):
        at = pl.ds(pl.multiple_of(((zz * HALVES + h) * 2 + c) * half + p * piece_rows, piece_rows), piece_rows)
        return pltpu.make_async_remote_copy(
            src_ref=gathered.at[at], dst_ref=gathered.at[at],
            send_sem=line_send, recv_sem=line_recv.at[(zz * HALVES + h) * PIECES + p],
            device_id=(peer, chan), device_id_type=MESH,
        )

    def sib_copy(h, zz, core):
        at = pl.ds(pl.multiple_of(((zz * HALVES + h) * 2 + core) * half, half), half)
        return pltpu.make_async_remote_copy(
            src_ref=gathered.at[at], dst_ref=gathered.at[at],
            send_sem=sib_send, recv_sem=sib_recv.at[zz * HALVES + h],
            device_id=(sib, chan), device_id_type=MESH,
        )

    for h in range(HALVES):
        gate_half(h)
        for p in range(PIECES):
            pl.when(has_right)(line_copy(h, p, z, me + SLAB).start)
            pl.when(has_left)(line_copy(h, p, z, me - SLAB).start)
        sib_copy(h, z, c).start()
    loads[6].wait()

    def source(g, sign):
        d = g // HALVES
        zz = z - d if sign < 0 else z + d
        there = jnp.logical_and(zz >= 0, zz < line)
        if sign > 0:
            there = jnp.logical_and(there, d > 0)
        return g % HALVES, zz, there

    def relay(g):
        for p in range(PIECES):
            for sign in (-1, 1):
                h, zz, there = source(g, sign)

                @pl.when(there)
                def _():
                    line_copy(h, p, zz, sib).wait_recv()
                    pl.when(has_right if sign < 0 else has_left)(line_copy(h, p, zz, me - SLAB * sign).start)
                    if p == PIECES - 1:
                        sib_copy(h, zz, c).start()

    def unit_at(h, zz, other, part):
        rows = pl.multiple_of((zz * HALVES + h) * 2 * half, 2 * half)
        at = pl.ds(part * cols, cols) if other else slice(None)
        return rows, at, (zz * HALVES + h) * (1 + parts) + (1 + part if other else 0)

    def cross_copy(h, zz, other, part, sender, target):
        rows, at, unit = unit_at(h, zz, other, part)
        rows = pl.ds(rows, 2 * half)
        return pltpu.make_async_remote_copy(
            src_ref=partial.at[other, rows, at], dst_ref=arrived.at[sender, other, rows, at],
            send_sem=cross_send, recv_sem=cross_recv.at[sender - (sender > target).astype(jnp.int32), unit],
            device_id=(me, target), device_id_type=MESH,
        )

    def compute(g, other, part):
        for sign in (-1, 1):
            h, zz, there = source(g, sign)

            @pl.when(there)
            def _():
                rows, at, _ = unit_at(h, zz, other, part)
                if not other:
                    sib_copy(h, zz, 1 - c).wait_recv()
                weights = w_other if other else w_ref
                partial[other, pl.ds(rows, 2 * half), at] = jnp.dot(
                    gathered[pl.ds(rows, 2 * half)], weights[:, at], preferred_element_type=F32
                ).astype(BF16)

                @pl.when(jnp.logical_not(owner_plane))
                def _():
                    cross_copy(h, zz, other, part, chan, out_chan).start()

    def finish(g, other, part):
        for sign in (-1, 1):
            h, zz, there = source(g, sign)

            @pl.when(jnp.logical_and(there, owner_plane))
            def _():
                rows, at, _ = unit_at(h, zz, other, part)
                total = partial[other, pl.ds(rows, 2 * half), at].astype(F32)
                for turn in range(1, n_chan):
                    sender = lax.rem(chan + turn, n_chan)
                    cross_copy(h, zz, other, part, sender, chan).wait_recv()
                    total = total + arrived[sender, other, pl.ds(rows, 2 * half), at].astype(F32)
                summed[other, pl.ds(rows, 2 * half), at] = total.astype(BF16)
                place = lax.rem(across if other else me, per_chan)
                for core in range(2):
                    to = zz * SLAB + x * 2 + core
                    src = summed.at[other, pl.ds(rows + core * half, half), at]
                    rows_to = pl.ds(pl.multiple_of(h * half, half), half)
                    if direct:
                        start = pl.multiple_of(place * width + part * cols, LANES)
                        dst = out_hbm.at[rows_to, pl.ds(start, cols if other else width)]
                    else:
                        dst = landed.at[place, rows_to, at]
                    remote = pltpu.make_async_remote_copy(
                        src_ref=src, dst_ref=dst, send_sem=part_send, recv_sem=part_recv,
                        device_id=(to, chan), device_id_type=MESH,
                    )
                    here = pltpu.make_async_copy(src, dst, part_recv)
                    pl.when(to == me)(here.start)
                    pl.when(to != me)(remote.start)

    def each(first, last, body):
        def run(g, _):
            body(g)
            return 0

        lax.fori_loop(first, last, run, 0)

    last = line * HALVES - 1
    split = min(2 * HALVES, last)

    def first_steps(g):
        pl.when(g >= HALVES)(lambda: relay(g))
        compute(g, 0, 0)
        pl.when(g >= 1)(lambda: finish(g - 1, 0, 0))

    each(0, split, first_steps)
    swapped(0).wait_recv()
    each(0, split, lambda g: compute(g, 1, 0))
    finish(split - 1, 0, 0)

    def later_steps(g):
        relay(g)
        compute(g, 0, 0)
        compute(g, 1, 0)

        @pl.when(g == split)
        def _():
            each(0, split, lambda e: finish(e, 1, 0))

        @pl.when(g > split)
        def _():
            finish(g - 1, 0, 0)
            finish(g - 1, 1, 0)

    each(split, last, later_steps)
    for part in range(1, parts):
        swapped(part).wait_recv()
    if parts > 1:
        each(0, last, lambda g: [compute(g, 1, part) for part in range(1, parts)])
    if last > split:
        finish(last - 1, 0, 0)
        finish(last - 1, 1, 0)
    else:
        each(0, split, lambda e: finish(e, 1, 0))
    if last >= HALVES:
        relay(last)
    compute(last, 0, 0)
    for part in range(parts):
        compute(last, 1, part)
    if parts > 1:
        each(0, last, lambda g: [finish(g, 1, part) for part in range(1, parts)])
    finish(last, 0, 0)
    for part in range(parts):
        finish(last, 1, part)

    def drained(ref, sem):
        return pltpu.make_async_remote_copy(
            src_ref=ref, dst_ref=ref, send_sem=sem, recv_sem=sem, device_id=(sib, chan), device_id_type=MESH,
        )

    if direct:
        drained(out_hbm, part_recv).wait_recv()
    else:
        drained(landed, part_recv).wait_recv()
        for i in range(per_chan):
            out_ref[:, i * width:(i + 1) * width] = landed[i]
        store = pltpu.make_async_copy(out_ref, out_hbm, load_sem.at[0])
        store.start()
        store.wait()

    drained(ends_all.at[pl.ds(0, SLAB - 1)], end_send).wait_send()
    drained(starts_all.at[pl.ds(0, SLAB - 1)], start_send).wait_send()
    for hop in range(1, line):
        pl.when(z + hop < line)(carry_copy(hop).wait_send)
    for part in range(parts):
        swapped(part).wait_send()
    inner = jnp.logical_and(has_left, has_right)
    if line > 2:
        pl.when(inner)(drained(gathered.at[pl.ds(0, (line + 1) * tok)], line_send).wait_send)
    if line > 1:
        pl.when(jnp.logical_not(inner))(drained(gathered.at[pl.ds(0, tok)], line_send).wait_send)
    drained(gathered.at[pl.ds(0, line * tok)], sib_send).wait_send()
    pl.when(owner_plane)(drained(summed.at[:, pl.ds(0, (2 * line - 1) * tok)], part_send).wait_send)
    pl.when(jnp.logical_not(owner_plane))(drained(partial, cross_send).wait_send)


def solution(mesh):
    n, n_chan = mesh.shape["seq"], mesh.shape["chan"]
    assert n % SLAB == 0 and n % (SLAB * n_chan) == 0

    def body(gate_input, key_input, value_input, decay_rate, residue, skip_gain, out_weight):
        tok, chans = gate_input.shape
        modes = decay_rate.shape[0]
        width = out_weight.shape[1]
        line = n // SLAB
        parts = column_parts(width)
        quarter = modes * chans // (LANES * SLAB)
        rows = 2 * line * tok
        units = line * HALVES * (1 + parts)
        direct = width % LANES == 0
        hbm = pl.BlockSpec(memory_space=pltpu.HBM)
        dma = pltpu.SemaphoreType.DMA
        slab_states = pltpu.VMEM((SLAB, quarter, LANES), BF16)
        all_states = pltpu.VMEM((SLAB * quarter, LANES), BF16)
        return pl.pallas_call(
            functools.partial(kernel, n, n_chan),
            out_shape=jax.ShapeDtypeStruct((tok, width * (n // n_chan)), BF16),
            in_specs=[hbm] * 7,
            out_specs=pl.BlockSpec(memory_space=pl.ANY),
            scratch_shapes=[
                pltpu.VMEM((tok, chans), BF16),
                pltpu.VMEM((tok, chans), BF16),
                pltpu.VMEM((tok, chans), BF16),
                pltpu.VMEM((modes, chans), F32),
                pltpu.VMEM((modes, chans), F32),
                pltpu.VMEM((1, chans), F32),
                pltpu.VMEM((chans, width), BF16),
                pltpu.VMEM((chans, width), BF16),
                dma((7,)), dma((parts,)), dma((parts,)),
                pltpu.VMEM((tok, chans), F32),
                pltpu.VMEM((tok, chans), F32),
                pltpu.VMEM((tok + SUB, LANES), F32),
                all_states, slab_states, pltpu.VMEM((line, quarter, LANES), BF16), pltpu.VMEM((quarter, LANES), BF16),
                slab_states, all_states,
                pltpu.VMEM((rows, chans), BF16),
                pltpu.VMEM((2, rows, width), BF16),
                pltpu.VMEM((n_chan, 2, rows, width), BF16),
                pltpu.VMEM((2, rows, width), BF16),
                pltpu.VMEM((1, 16, LANES) if direct else (n // n_chan, tok, width), BF16),
                pltpu.VMEM((16, LANES) if direct else (tok, width * (n // n_chan)), BF16),
                pltpu.SemaphoreType.REGULAR, dma(()), dma(()), dma((line,)), dma((line,)), dma(()), dma(()),
                dma(()), dma((line * HALVES * PIECES,)), dma(()), dma((line * HALVES,)),
                dma(()), dma((max(n_chan - 1, 1), units)), dma(()), dma(()),
            ],
            compiler_params=pltpu.CompilerParams(
                collective_id=0, has_side_effects=True, vmem_limit_bytes=40 * 2**20
            ),
            cost_estimate=pl.CostEstimate(
                flops=2 * n * tok * chans * width, bytes_accessed=4 * tok * chans, transcendentals=0
            ),
        )(*[
            pltpu.with_memory_space_constraint(array, pltpu.HBM)
            for array in (
                gate_input, key_input, value_input, decay_rate, residue, skip_gain.reshape(1, chans), out_weight
            )
        ])

    return jax.shard_map(
        body,
        mesh=mesh,
        in_specs=(
            P("seq", "chan"),
            P("seq", "chan"),
            P("seq", "chan"),
            P(None, "chan"),
            P(None, "chan"),
            P("chan"),
            P("chan", "seq"),
        ),
        out_specs=P("seq", "chan"),
        check_vma=False,
    )
```

```python
import functools

import jax
import jax.numpy as jnp
from jax import lax
from jax.experimental import pallas as pl
from jax.experimental.pallas import tpu as pltpu
from jax.sharding import PartitionSpec as P

MESH = pl.DeviceIdType.MESH
F32 = jnp.float32
BF16 = jnp.bfloat16
LANES = 128
SUB = 8
SLAB = 4
HALVES = 2


def one_minus_exp(y):
    series = jnp.ones_like(y)
    for order in range(10, 1, -1):
        series = 1.0 - y * (1.0 / order) * series
    return jnp.where(y < 0.4, y * series, 1.0 - jnp.exp(-y))


def column_parts(width):
    return 2 if width % (2 * LANES) == 0 else 1


def kernel(
    n, n_chan,
    q_hbm, k_hbm, v_hbm, rate_hbm, residue_hbm, skip_hbm, w_hbm, out_hbm,
    q_ref, k_ref, v_ref, rate_ref, amp_ref, skip_ref, w_ref, w_other, load_sem, w_send, w_recv,
    sig, local, padded, ends, ends_all, carry_in, carry_out, starts_all, starts,
    local_out, q_near, local_near, starts_near, gathered, partial,
    ready, end_send, end_recv, carry_send, carry_recv, start_send, start_recv,
    near_send, near_recv, line_send, line_recv, sib_send, sib_recv, part_send, part_recv,
):
    loads = [
        pltpu.make_async_copy(source, target, load_sem.at[i])
        for i, (source, target) in enumerate([
            (k_hbm, k_ref), (v_hbm, v_ref), (rate_hbm, rate_ref),
            (residue_hbm, amp_ref), (skip_hbm, skip_ref), (q_hbm, q_ref), (w_hbm, w_ref),
        ])
    ]
    for load in loads:
        load.start()
    tok, chans = q_ref.shape
    modes = rate_ref.shape[0]
    blocks = chans // LANES
    width = w_ref.shape[1]
    per_chan = n // n_chan
    line = n // SLAB
    tiles = tok // SUB
    quarter_blocks = blocks // SLAB
    quarter = quarter_blocks * modes
    half = tok // HALVES
    parts = column_parts(width)
    cols = width // parts
    direct = width % LANES == 0

    me = lax.axis_index("seq")
    chan = lax.axis_index("chan")
    z = me // SLAB
    x = (me // 2) % 2
    c = me % 2
    qd = me % SLAB
    sib = me + 1 - 2 * c
    across = me + 2 - 4 * x
    has_right = z < line - 1
    has_left = z > 0
    out_chan = me // per_chan
    owner_plane = chan == out_chan
    giver = jnp.logical_or(z == 1, z == line - 2)
    taker = jnp.logical_not(jnp.logical_and(has_left, has_right))
    near = jnp.where(z == 0, 1, line - 2)
    taken_by = jnp.where(z == 1, me - SLAB, me + SLAB)

    def quarter_of(turn):
        return (x if turn < 2 else 1 - x) * 2 + (c if turn % 2 == 0 else 1 - c)

    def mate(turn):
        return me - qd + quarter_of(turn)

    barrier = pltpu.get_barrier_semaphore()

    def hello(seq, ch):
        pl.semaphore_signal(barrier, inc=1, device_id=(seq, ch), device_id_type=MESH)

    for turn in range(1, SLAB):
        hello(mate(turn), chan)
    pl.when(has_right)(lambda: hello(me + SLAB, chan))
    pl.when(has_left)(lambda: hello(me - SLAB, chan))
    for turn in range(1, n_chan):
        hello(me, lax.rem(chan + turn, n_chan))
    greeters = SLAB - 1 + n_chan - 1 + has_right.astype(jnp.int32) + has_left.astype(jnp.int32)
    steps = lax.broadcasted_iota(jnp.int32, (SUB, LANES), 0).astype(F32)

    def lanes(b):
        return pl.ds(pl.multiple_of(b * LANES, LANES), LANES)

    for load in loads[:3]:
        load.wait()

    def end_block(b, _):
        at = lanes(b)
        s = k_ref[:, at].astype(F32) * v_ref[:, at].astype(F32)
        sig[:, at] = s
        found = []
        for m in range(modes):
            rate = rate_ref[pl.ds(m, 1), at]
            jump = jnp.exp(-float(SUB) * rate)
            total = s[:SUB]
            for t in range(1, tiles):
                total = total * jump + s[t * SUB:(t + 1) * SUB]
            total = total * jnp.exp(-rate * (float(SUB - 1) - steps))
            found.append(jnp.sum(total, axis=0, keepdims=True))
        ends[pl.ds(pl.multiple_of(b * modes, modes), modes)] = jnp.concatenate(found, axis=0).astype(BF16)
        return 0

    lax.fori_loop(0, blocks, end_block, 0)

    pl.semaphore_wait(barrier, greeters)

    def quarter_rows(p):
        return pl.ds(pl.multiple_of(p * quarter, quarter), quarter)

    def slab_copy(source, target, send_sem, recv_sem, turn):
        return pltpu.make_async_remote_copy(
            src_ref=source, dst_ref=target, send_sem=send_sem, recv_sem=recv_sem,
            device_id=(mate(turn), chan), device_id_type=MESH,
        )

    def slab_wait(ref, sem):
        return slab_copy(ref, ref, sem, sem, 1)

    for turn in (2, 3, 1):
        slab_copy(ends.at[quarter_rows(quarter_of(turn))], ends_all.at[qd], end_send, end_recv, turn).start()
    ends_all[qd] = ends[quarter_rows(qd)]

    def near_copy(source, target, kind):
        return pltpu.make_async_remote_copy(
            src_ref=source, dst_ref=target, send_sem=near_send.at[kind], recv_sem=near_recv.at[kind],
            device_id=(taken_by, chan), device_id_type=MESH,
        )

    def give_q(first, rows):
        near_copy(q_hbm.at[pl.ds(first, rows)], q_near.at[pl.ds(first, rows)], 0).start()

    early_rows = tok * 3 // 4
    pl.when(giver)(lambda: give_q(0, early_rows))

    def swap(part, first, rows):
        at = (pl.ds(first, rows), pl.ds(part * cols, cols))
        pltpu.make_async_remote_copy(
            src_ref=w_hbm.at[at], dst_ref=w_other.at[at],
            send_sem=w_send.at[part], recv_sem=w_recv.at[part],
            device_id=(across, chan), device_id_type=MESH,
        ).start()

    def swapped(part):
        at = (slice(None), pl.ds(part * cols, cols))
        return pltpu.make_async_remote_copy(
            src_ref=w_other.at[at], dst_ref=w_other.at[at],
            send_sem=w_send.at[part], recv_sem=w_recv.at[part],
            device_id=(across, chan), device_id_type=MESH,
        )

    block_rows = LANES // 4
    middle_rows = chans * 7 // 32

    loads[3].wait()
    loads[4].wait()
    amp_ref[...] = amp_ref[...] * jnp.sqrt(one_minus_exp(2.0 * rate_ref[...]))

    padded[:SUB] = jnp.zeros((SUB, LANES), F32)

    def local_block(b, _):
        swap(0, pl.multiple_of(b * block_rows, block_rows), block_rows)
        at = lanes(b)
        response = [jnp.zeros((SUB, LANES), F32)] * tiles
        for m in range(modes):
            rate = rate_ref[pl.ds(m, 1), at]
            jump = jnp.exp(-float(SUB) * rate)
            term = amp_ref[pl.ds(m, 1), at] * jnp.exp(-rate * steps)
            for t in range(tiles):
                response[t] = response[t] + term
                if t < tiles - 1:
                    term = term * jump
        padded[SUB:] = jnp.concatenate(response, axis=0)
        skip = skip_ref[:, at]
        totals = [skip * sig[t * SUB:(t + 1) * SUB, at] for t in range(tiles)]
        for lag in range(SUB):
            moved = [padded[pl.ds(SUB - lag + t * SUB, SUB)] for t in range(tiles)]
            for first in range(tiles):
                value = sig[pl.ds(first * SUB + lag, 1), at]
                for t in range(first, tiles):
                    totals[t] = totals[t] + moved[t - first] * value
        totals = jnp.concatenate(totals, axis=0)
        local[:, at] = totals
        local_out[:, at] = totals.astype(BF16)
        return 0

    lax.fori_loop(0, blocks, local_block, 0)

    def signal_left():
        pl.semaphore_signal(ready, inc=1, device_id=(me - SLAB, chan), device_id_type=MESH)

    pl.when(z < line - 2)(lambda: pl.semaphore_wait(ready, 1))
    pl.when(jnp.logical_and(has_left, has_right))(signal_left)

    fades = jnp.concatenate(
        [jnp.exp(-float(tok) * rate_ref[:, lanes(qd * quarter_blocks + j)]) for j in range(quarter_blocks)], axis=0
    )
    slab_wait(ends_all.at[pl.ds(0, SLAB - 1)], end_recv).wait_recv()
    found = [ends_all[p].astype(F32) for p in range(SLAB)]
    slab_total = found[0]
    for p in range(1, SLAB):
        slab_total = slab_total * fades + found[p]
    slab_fade = (fades * fades) * (fades * fades)

    def carry_copy(hop):
        return pltpu.make_async_remote_copy(
            src_ref=carry_out, dst_ref=carry_in.at[z], send_sem=carry_send.at[hop - 1], recv_sem=carry_recv.at[z],
            device_id=(me + hop * SLAB, chan), device_id_type=MESH,
        )

    @pl.when(has_right)
    def _():
        carry_out[...] = slab_total.astype(BF16)
        for hop in range(1, line):
            pl.when(z + hop < line)(carry_copy(hop).start)

    @pl.when(giver)
    def _():
        give_q(early_rows, tok - early_rows)
        near_copy(local_out, local_near, 1).start()

    @pl.when(has_left)
    def _():
        swap(0, blocks * block_rows, middle_rows)

    def collect(i, carry):
        pltpu.make_async_remote_copy(
            src_ref=carry_in.at[i], dst_ref=carry_in.at[i], send_sem=carry_send.at[0], recv_sem=carry_recv.at[i],
            device_id=(sib, chan), device_id_type=MESH,
        ).wait_recv()
        return carry * slab_fade + carry_in[i].astype(F32)

    carry = lax.fori_loop(0, z, collect, jnp.zeros((quarter, LANES), F32))

    state = carry
    for p in range(SLAB):
        starts_all[p] = state.astype(BF16)
        if p < SLAB - 1:
            state = state * fades + found[p]
    for turn in (2, 3, 1):
        slab_copy(
            starts_all.at[quarter_of(turn)], starts.at[quarter_rows(qd)], start_send, start_recv.at[turn - 1], turn
        ).start()
    starts[quarter_rows(qd)] = starts_all[qd]

    @pl.when(jnp.logical_not(has_left))
    def _():
        swap(0, blocks * block_rows, middle_rows)

    swap(0, blocks * block_rows + middle_rows, chans - blocks * block_rows - middle_rows)
    for part in range(1, parts):
        swap(part, 0, chans)
    loads[5].wait()

    def gate(zz, q_from, local_from, starts_from, first, count):
        targets = [
            pl.ds(pl.multiple_of(((zz * HALVES + h) * 2 + c) * half, half), half) for h in range(HALVES)
        ]

        def gate_block(b, _):
            at = lanes(b)
            held = starts_from[pl.ds(pl.multiple_of(b * modes, modes), modes)].astype(F32)
            found = local_from[:, at].astype(F32)
            totals = [found[t * SUB:(t + 1) * SUB] for t in range(tiles)]
            for m in range(modes):
                rate = rate_ref[pl.ds(m, 1), at]
                jump = jnp.exp(-float(SUB) * rate)
                term = (amp_ref[pl.ds(m, 1), at] * held[m:m + 1]) * jnp.exp(-rate * (steps + 1.0))
                for t in range(tiles):
                    totals[t] = totals[t] + term
                    if t < tiles - 1:
                        term = term * jump
            gated = (q_from[:, at].astype(F32) * jnp.concatenate(totals, axis=0)).astype(BF16)
            for h in range(HALVES):
                gathered[targets[h], at] = gated[h * half:(h + 1) * half]
            return 0

        lax.fori_loop(first, first + count, gate_block, 0)

    quarter_cols = chans // SLAB

    def line_copy(h, turn, zz, peer):
        at = (
            pl.ds(pl.multiple_of(((zz * HALVES + h) * 2 + c) * half, half), half),
            pl.ds(pl.multiple_of(quarter_of(turn) * quarter_cols, quarter_cols), quarter_cols),
        )
        return pltpu.make_async_remote_copy(
            src_ref=gathered.at[at], dst_ref=gathered.at[at],
            send_sem=line_send, recv_sem=line_recv.at[(zz * HALVES + h) * SLAB + turn],
            device_id=(peer, chan), device_id_type=MESH,
        )

    def sib_copy(h, zz, core):
        at = pl.ds(pl.multiple_of(((zz * HALVES + h) * 2 + core) * half, half), half)
        return pltpu.make_async_remote_copy(
            src_ref=gathered.at[at], dst_ref=gathered.at[at],
            send_sem=sib_send, recv_sem=sib_recv.at[zz * HALVES + h],
            device_id=(sib, chan), device_id_type=MESH,
        )

    def send_own(pieces):
        for h, turn in pieces:
            pl.when(jnp.logical_and(has_right, z != line - 2))(line_copy(h, turn, z, me + SLAB).start)
            pl.when(jnp.logical_and(has_left, z != 1))(line_copy(h, turn, z, me - SLAB).start)

    order = [[(0, 0), (1, 0), (0, 1), (1, 1), (0, 2), (0, 3)], [(1, 2), (1, 3)]]
    for turn in range(SLAB):
        if turn:
            slab_wait(starts.at[quarter_rows(quarter_of(turn))], start_recv.at[turn - 1]).wait_recv()
        gate(z, q_ref, local, starts, quarter_of(turn) * quarter_blocks, quarter_blocks)
        if turn < 2:
            send_own(order[0][2 * turn:2 * turn + 2])
    pl.when(giver)(near_copy(starts, starts_near, 2).start)
    send_own(order[0][4:] + order[1])
    for h in range(HALVES):
        sib_copy(h, z, c).start()
    loads[6].wait()

    def source(d, sign):
        zz = z - d if sign < 0 else z + d
        there = jnp.logical_and(zz >= 0, zz < line)
        if sign > 0:
            there = jnp.logical_and(there, d > 0)
        return zz, there

    def relay(d, h):
        taking = jnp.logical_and(taker, d == 1)
        if h == 0:
            @pl.when(taking)
            def _():
                near_copy(q_near, q_near, 0).wait_recv()
                near_copy(local_near, local_near, 1).wait_recv()
                near_copy(starts_near, starts_near, 2).wait_recv()
                gate(near, q_near, local_near, starts_near, 0, blocks)
                for e in range(HALVES):
                    sib_copy(e, near, c).start()

        for e, turn in order[h]:
            for sign in (-1, 1):
                zz, there = source(d, sign)

                @pl.when(jnp.logical_and(there, jnp.logical_not(taking)))
                def _():
                    line_copy(e, turn, zz, sib).wait_recv()
                    pl.when(has_right if sign < 0 else has_left)(line_copy(e, turn, zz, me - SLAB * sign).start)
                    if (e, turn) == order[h][-1]:
                        sib_copy(h, zz, c).start()

    def compute(d, halves, other, part):
        for sign in (-1, 1):
            zz, there = source(d, sign)

            @pl.when(there)
            def _():
                if not other:
                    for h in halves:
                        sib_copy(h, zz, 1 - c).wait_recv()
                size = 2 * half * len(halves)
                rows = pl.ds(pl.multiple_of((zz * HALVES + halves[0]) * 2 * half, 2 * half), size)
                at = pl.ds(part * cols, cols) if other else slice(None)
                weights = w_other if other else w_ref
                partial[other, rows, at] = jnp.dot(
                    gathered[rows], weights[:, at], preferred_element_type=F32
                ).astype(BF16)
                place = lax.rem(across if other else me, per_chan)
                for h in halves:
                    for core in range(2):
                        to = zz * SLAB + x * 2 + core
                        sent = pl.ds(pl.multiple_of(((zz * HALVES + h) * 2 + core) * half, half), half)
                        src = partial.at[other, sent, at]
                        if direct:
                            start = pl.multiple_of(place * width + part * cols, LANES)
                            dst = out_hbm.at[chan, pl.ds(h * half, half), pl.ds(start, cols if other else width)]
                        else:
                            dst = out_hbm.at[chan, place, pl.ds(h * half, half), at]
                        remote = pltpu.make_async_remote_copy(
                            src_ref=src, dst_ref=dst, send_sem=part_send, recv_sem=part_recv,
                            device_id=(to, out_chan), device_id_type=MESH,
                        )
                        here = pltpu.make_async_copy(src, dst, part_recv)
                        stays = jnp.logical_and(to == me, owner_plane)
                        pl.when(stays)(here.start)
                        pl.when(jnp.logical_not(stays))(remote.start)

    def each(first, last, body):
        def run(g, _):
            body(g)
            return 0

        lax.fori_loop(first, last, run, 0)

    last = line - 1
    split = 2
    whole = tuple(range(HALVES))

    compute(0, whole, 0, 0)

    def relay_whole(d):
        for h in range(HALVES):
            relay(d, h)

    relay_whole(1)
    swapped(0).wait_recv()
    compute(0, whole, 1, 0)
    each(split, last, relay_whole)

    def later_steps(d):
        compute(d, whole, 0, 0)
        compute(d, whole, 1, 0)

    each(1, last, later_steps)
    for h in range(HALVES):
        relay(last, h)
    for part in range(1, parts):
        swapped(part).wait_recv()
        each(0, last, lambda d: compute(last - 1 - d, whole, 1, part))
    compute(last, whole, 0, 0)
    for part in range(parts):
        compute(last, whole, 1, part)

    def drained(ref, sem):
        return pltpu.make_async_remote_copy(
            src_ref=ref, dst_ref=ref, send_sem=sem, recv_sem=sem, device_id=(sib, chan), device_id_type=MESH,
        )

    drained(out_hbm, part_recv).wait_recv()

    drained(ends_all.at[pl.ds(0, SLAB - 1)], end_send).wait_send()
    drained(starts_all.at[pl.ds(0, SLAB - 1)], start_send).wait_send()
    for hop in range(1, line):
        pl.when(z + hop < line)(carry_copy(hop).wait_send)
    for part in range(parts):
        swapped(part).wait_send()
    inner = jnp.logical_not(jnp.logical_or(taker, giver))
    pl.when(inner)(drained(gathered.at[pl.ds(0, (line + 1) * tok)], line_send).wait_send)
    pl.when(taker)(drained(gathered.at[pl.ds(0, tok)], line_send).wait_send)
    pl.when(giver)(drained(gathered.at[pl.ds(0, line * tok)], line_send).wait_send)
    for kind, ref in enumerate((q_near, local_near, starts_near)):
        pl.when(giver)(near_copy(ref, ref, kind).wait_send)
    drained(gathered.at[pl.ds(0, line * tok)], sib_send).wait_send()
    pl.when(owner_plane)(drained(partial.at[:, pl.ds(0, (2 * line - 1) * tok)], part_send).wait_send)
    pl.when(jnp.logical_not(owner_plane))(drained(partial, part_send).wait_send)


def solution(mesh):
    n, n_chan = mesh.shape["seq"], mesh.shape["chan"]
    assert n % (SLAB * n_chan) == 0 and n >= 4 * SLAB

    def body(gate_input, key_input, value_input, decay_rate, residue, skip_gain, out_weight):
        tok, chans = gate_input.shape
        modes = decay_rate.shape[0]
        width = out_weight.shape[1]
        line = n // SLAB
        quarter = modes * chans // (LANES * SLAB)
        rows = 2 * line * tok
        direct = width % LANES == 0
        hbm = pl.BlockSpec(memory_space=pltpu.HBM)
        dma = pltpu.SemaphoreType.DMA
        slab_states = pltpu.VMEM((SLAB, quarter, LANES), BF16)
        all_states = pltpu.VMEM((SLAB * quarter, LANES), BF16)
        per_chan = n // n_chan
        landing = (n_chan, tok, width * per_chan) if direct else (n_chan, per_chan, tok, width)
        landed = pl.pallas_call(
            functools.partial(kernel, n, n_chan),
            out_shape=jax.ShapeDtypeStruct(landing, BF16),
            in_specs=[hbm] * 7,
            out_specs=pl.BlockSpec(memory_space=pl.ANY),
            scratch_shapes=[
                pltpu.VMEM((tok, chans), BF16),
                pltpu.VMEM((tok, chans), BF16),
                pltpu.VMEM((tok, chans), BF16),
                pltpu.VMEM((modes, chans), F32),
                pltpu.VMEM((modes, chans), F32),
                pltpu.VMEM((1, chans), F32),
                pltpu.VMEM((chans, width), BF16),
                pltpu.VMEM((chans, width), BF16),
                dma((7,)), dma((column_parts(width),)), dma((column_parts(width),)),
                pltpu.VMEM((tok, chans), F32),
                pltpu.VMEM((tok, chans), F32),
                pltpu.VMEM((tok + SUB, LANES), F32),
                all_states, slab_states, pltpu.VMEM((line, quarter, LANES), BF16), pltpu.VMEM((quarter, LANES), BF16),
                slab_states, all_states,
                pltpu.VMEM((tok, chans), BF16), pltpu.VMEM((tok, chans), BF16), pltpu.VMEM((tok, chans), BF16), all_states,
                pltpu.VMEM((rows, chans), BF16),
                pltpu.VMEM((2, rows, width), BF16),
                pltpu.SemaphoreType.REGULAR, dma(()), dma(()), dma((line,)), dma((line,)), dma(()), dma((SLAB - 1,)),
                dma((3,)), dma((3,)), dma(()), dma((line * HALVES * SLAB,)), dma(()), dma((line * HALVES,)),
                dma(()), dma(()),
            ],
            compiler_params=pltpu.CompilerParams(
                collective_id=0, has_side_effects=True, vmem_limit_bytes=40 * 2**20
            ),
            cost_estimate=pl.CostEstimate(
                flops=2 * n * tok * chans * width, bytes_accessed=4 * tok * chans, transcendentals=0
            ),
        )(*[
            pltpu.with_memory_space_constraint(array, pltpu.HBM)
            for array in (
                gate_input, key_input, value_input, decay_rate, residue, skip_gain.reshape(1, chans), out_weight
            )
        ])
        mixed = landed[0].astype(F32)
        for j in range(1, n_chan):
            mixed = mixed + landed[j].astype(F32)
        mixed = mixed.astype(BF16)
        return mixed if direct else mixed.transpose(1, 0, 2).reshape(tok, width * per_chan)

    return jax.shard_map(
        body,
        mesh=mesh,
        in_specs=(
            P("seq", "chan"),
            P("seq", "chan"),
            P("seq", "chan"),
            P(None, "chan"),
            P(None, "chan"),
            P("chan"),
            P("chan", "seq"),
        ),
        out_specs=P("seq", "chan"),
        check_vma=False,
    )
```

```python
import functools

import jax
import jax.numpy as jnp
from jax import lax
from jax.experimental import pallas as pl
from jax.experimental.pallas import tpu as pltpu
from jax.sharding import PartitionSpec as P

MESH = pl.DeviceIdType.MESH
F32 = jnp.float32
BF16 = jnp.bfloat16
LANES = 128
SUB = 8
SLAB = 4
HALVES = 2


def one_minus_exp(y):
    series = jnp.ones_like(y)
    for order in range(10, 1, -1):
        series = 1.0 - y * (1.0 / order) * series
    return jnp.where(y < 0.4, y * series, 1.0 - jnp.exp(-y))


def column_parts(width):
    return 2 if width % (2 * LANES) == 0 else 1


def kernel(
    n, n_chan,
    q_hbm, k_hbm, v_hbm, rate_hbm, residue_hbm, skip_hbm, w_hbm, out_hbm,
    q_ref, k_ref, v_ref, rate_ref, amp_ref, skip_ref, w_ref, w_other, load_sem, w_send, w_recv,
    sig, local, padded, ends, ends_all, carry_in, carry_out, starts_all, starts,
    local_out, q_near, local_near, starts_near, gathered, partial,
    ready, end_send, end_recv, carry_send, carry_recv, start_send, start_recv,
    near_send, near_recv, line_send, line_recv, sib_send, sib_recv, part_send, part_recv,
):
    loads = [
        pltpu.make_async_copy(source, target, load_sem.at[i])
        for i, (source, target) in enumerate([
            (k_hbm, k_ref), (v_hbm, v_ref), (rate_hbm, rate_ref),
            (residue_hbm, amp_ref), (skip_hbm, skip_ref), (q_hbm, q_ref), (w_hbm, w_ref),
        ])
    ]
    for load in loads:
        load.start()
    tok, chans = q_ref.shape
    modes = rate_ref.shape[0]
    blocks = chans // LANES
    width = w_ref.shape[1]
    per_chan = n // n_chan
    line = n // SLAB
    tiles = tok // SUB
    quarter_blocks = blocks // SLAB
    quarter = quarter_blocks * modes
    half = tok // HALVES
    parts = column_parts(width)
    cols = width // parts
    direct = width % LANES == 0

    me = lax.axis_index("seq")
    chan = lax.axis_index("chan")
    z = me // SLAB
    x = (me // 2) % 2
    c = me % 2
    qd = me % SLAB
    sib = me + 1 - 2 * c
    across = me + 2 - 4 * x
    has_right = z < line - 1
    has_left = z > 0
    out_chan = me // per_chan
    owner_plane = chan == out_chan
    giver = jnp.logical_or(z == 1, z == line - 2)
    taker = jnp.logical_not(jnp.logical_and(has_left, has_right))
    near = jnp.where(z == 0, 1, line - 2)
    taken_by = jnp.where(z == 1, me - SLAB, me + SLAB)

    def quarter_of(turn):
        return (x if turn < 2 else 1 - x) * 2 + (c if turn % 2 == 0 else 1 - c)

    def mate(turn):
        return me - qd + quarter_of(turn)

    barrier = pltpu.get_barrier_semaphore()

    def hello(seq, ch):
        pl.semaphore_signal(barrier, inc=1, device_id=(seq, ch), device_id_type=MESH)

    for turn in range(1, SLAB):
        hello(mate(turn), chan)
    pl.when(has_right)(lambda: hello(me + SLAB, chan))
    pl.when(has_left)(lambda: hello(me - SLAB, chan))
    for turn in range(1, n_chan):
        hello(me, lax.rem(chan + turn, n_chan))
    greeters = SLAB - 1 + n_chan - 1 + has_right.astype(jnp.int32) + has_left.astype(jnp.int32)
    steps = lax.broadcasted_iota(jnp.int32, (SUB, LANES), 0).astype(F32)

    def lanes(b):
        return pl.ds(pl.multiple_of(b * LANES, LANES), LANES)

    for load in loads[:3]:
        load.wait()

    def end_block(b, _):
        at = lanes(b)
        s = k_ref[:, at].astype(F32) * v_ref[:, at].astype(F32)
        sig[:, at] = s
        found = []
        for m in range(modes):
            rate = rate_ref[pl.ds(m, 1), at]
            jump = jnp.exp(-float(SUB) * rate)
            total = s[:SUB]
            for t in range(1, tiles):
                total = total * jump + s[t * SUB:(t + 1) * SUB]
            total = total * jnp.exp(-rate * (float(SUB - 1) - steps))
            found.append(jnp.sum(total, axis=0, keepdims=True))
        ends[pl.ds(pl.multiple_of(b * modes, modes), modes)] = jnp.concatenate(found, axis=0).astype(BF16)
        return 0

    lax.fori_loop(0, blocks, end_block, 0)

    pl.semaphore_wait(barrier, greeters)

    def quarter_rows(p):
        return pl.ds(pl.multiple_of(p * quarter, quarter), quarter)

    def slab_copy(source, target, send_sem, recv_sem, turn):
        return pltpu.make_async_remote_copy(
            src_ref=source, dst_ref=target, send_sem=send_sem, recv_sem=recv_sem,
            device_id=(mate(turn), chan), device_id_type=MESH,
        )

    def slab_wait(ref, sem):
        return slab_copy(ref, ref, sem, sem, 1)

    for turn in (2, 3, 1):
        slab_copy(ends.at[quarter_rows(quarter_of(turn))], ends_all.at[qd], end_send, end_recv, turn).start()
    ends_all[qd] = ends[quarter_rows(qd)]

    def near_copy(source, target, kind):
        return pltpu.make_async_remote_copy(
            src_ref=source, dst_ref=target, send_sem=near_send.at[kind], recv_sem=near_recv.at[kind],
            device_id=(taken_by, chan), device_id_type=MESH,
        )

    late_cols = pl.ds(pl.multiple_of((1 - x) * (chans // 2), chans // 2), chans // 2)
    late_states = pl.ds(pl.multiple_of((1 - x) * 2 * quarter, 2 * quarter), 2 * quarter)
    near_copies = [
        near_copy(q_hbm.at[:, late_cols], q_near.at[:, late_cols], 0),
        near_copy(local_out.at[:, late_cols], local_near.at[:, late_cols], 1),
        near_copy(starts.at[late_states], starts_near.at[late_states], 2),
    ]
    pl.when(giver)(near_copies[0].start)

    def swap(part, first, rows):
        at = (pl.ds(first, rows), pl.ds(part * cols, cols))
        pltpu.make_async_remote_copy(
            src_ref=w_hbm.at[at], dst_ref=w_other.at[at],
            send_sem=w_send.at[part], recv_sem=w_recv.at[part],
            device_id=(across, chan), device_id_type=MESH,
        ).start()

    def swapped(part):
        at = (slice(None), pl.ds(part * cols, cols))
        return pltpu.make_async_remote_copy(
            src_ref=w_other.at[at], dst_ref=w_other.at[at],
            send_sem=w_send.at[part], recv_sem=w_recv.at[part],
            device_id=(across, chan), device_id_type=MESH,
        )

    block_rows = LANES // 4
    middle_rows = chans * 7 // 32

    loads[3].wait()
    loads[4].wait()
    amp_ref[...] = amp_ref[...] * jnp.sqrt(one_minus_exp(2.0 * rate_ref[...]))

    padded[:SUB] = jnp.zeros((SUB, LANES), F32)

    def local_block(b, _):
        swap(0, pl.multiple_of(b * block_rows, block_rows), block_rows)
        at = lanes(b)
        response = [jnp.zeros((SUB, LANES), F32)] * tiles
        for m in range(modes):
            rate = rate_ref[pl.ds(m, 1), at]
            jump = jnp.exp(-float(SUB) * rate)
            term = amp_ref[pl.ds(m, 1), at] * jnp.exp(-rate * steps)
            for t in range(tiles):
                response[t] = response[t] + term
                if t < tiles - 1:
                    term = term * jump
        padded[SUB:] = jnp.concatenate(response, axis=0)
        skip = skip_ref[:, at]
        totals = [skip * sig[t * SUB:(t + 1) * SUB, at] for t in range(tiles)]
        for lag in range(SUB):
            moved = [padded[pl.ds(SUB - lag + t * SUB, SUB)] for t in range(tiles)]
            for first in range(tiles):
                value = sig[pl.ds(first * SUB + lag, 1), at]
                for t in range(first, tiles):
                    totals[t] = totals[t] + moved[t - first] * value
        totals = jnp.concatenate(totals, axis=0)
        local[:, at] = totals
        local_out[:, at] = totals.astype(BF16)
        return 0

    lax.fori_loop(0, blocks, local_block, 0)

    def signal_left():
        pl.semaphore_signal(ready, inc=1, device_id=(me - SLAB, chan), device_id_type=MESH)

    pl.when(z < line - 2)(lambda: pl.semaphore_wait(ready, 1))
    pl.when(jnp.logical_and(has_left, has_right))(signal_left)

    fades = jnp.concatenate(
        [jnp.exp(-float(tok) * rate_ref[:, lanes(qd * quarter_blocks + j)]) for j in range(quarter_blocks)], axis=0
    )
    slab_wait(ends_all.at[pl.ds(0, SLAB - 1)], end_recv).wait_recv()
    found = [ends_all[p].astype(F32) for p in range(SLAB)]
    slab_total = found[0]
    for p in range(1, SLAB):
        slab_total = slab_total * fades + found[p]
    slab_fade = (fades * fades) * (fades * fades)

    def carry_copy(hop):
        return pltpu.make_async_remote_copy(
            src_ref=carry_out, dst_ref=carry_in.at[z], send_sem=carry_send.at[hop - 1], recv_sem=carry_recv.at[z],
            device_id=(me + hop * SLAB, chan), device_id_type=MESH,
        )

    @pl.when(has_right)
    def _():
        carry_out[...] = slab_total.astype(BF16)
        for hop in range(1, line):
            pl.when(z + hop < line)(carry_copy(hop).start)

    pl.when(giver)(near_copies[1].start)

    @pl.when(has_left)
    def _():
        swap(0, blocks * block_rows, middle_rows)

    def collect(i, carry):
        pltpu.make_async_remote_copy(
            src_ref=carry_in.at[i], dst_ref=carry_in.at[i], send_sem=carry_send.at[0], recv_sem=carry_recv.at[i],
            device_id=(sib, chan), device_id_type=MESH,
        ).wait_recv()
        return carry * slab_fade + carry_in[i].astype(F32)

    carry = lax.fori_loop(0, z, collect, jnp.zeros((quarter, LANES), F32))

    state = carry
    for p in range(SLAB):
        starts_all[p] = state.astype(BF16)
        if p < SLAB - 1:
            state = state * fades + found[p]
    for turn in (2, 3, 1):
        slab_copy(
            starts_all.at[quarter_of(turn)], starts.at[quarter_rows(qd)], start_send, start_recv.at[turn - 1], turn
        ).start()
    starts[quarter_rows(qd)] = starts_all[qd]

    @pl.when(jnp.logical_not(has_left))
    def _():
        swap(0, blocks * block_rows, middle_rows)

    swap(0, blocks * block_rows + middle_rows, chans - blocks * block_rows - middle_rows)
    for part in range(1, parts):
        swap(part, 0, chans)
    loads[5].wait()

    def gate(zz, q_from, local_from, starts_from, first, count):
        targets = [
            pl.ds(pl.multiple_of(((zz * HALVES + h) * 2 + c) * half, half), half) for h in range(HALVES)
        ]

        def gate_block(b, _):
            at = lanes(b)
            held = starts_from[pl.ds(pl.multiple_of(b * modes, modes), modes)].astype(F32)
            found = local_from[:, at].astype(F32)
            totals = [found[t * SUB:(t + 1) * SUB] for t in range(tiles)]
            for m in range(modes):
                rate = rate_ref[pl.ds(m, 1), at]
                jump = jnp.exp(-float(SUB) * rate)
                term = (amp_ref[pl.ds(m, 1), at] * held[m:m + 1]) * jnp.exp(-rate * (steps + 1.0))
                for t in range(tiles):
                    totals[t] = totals[t] + term
                    if t < tiles - 1:
                        term = term * jump
            gated = (q_from[:, at].astype(F32) * jnp.concatenate(totals, axis=0)).astype(BF16)
            for h in range(HALVES):
                gathered[targets[h], at] = gated[h * half:(h + 1) * half]
            return 0

        lax.fori_loop(first, first + count, gate_block, 0)

    quarter_cols = chans // SLAB

    def line_copy(h, turn, zz, peer):
        at = (
            pl.ds(pl.multiple_of(((zz * HALVES + h) * 2 + c) * half, half), half),
            pl.ds(pl.multiple_of(quarter_of(turn) * quarter_cols, quarter_cols), quarter_cols),
        )
        return pltpu.make_async_remote_copy(
            src_ref=gathered.at[at], dst_ref=gathered.at[at],
            send_sem=line_send, recv_sem=line_recv.at[(zz * HALVES + h) * SLAB + turn],
            device_id=(peer, chan), device_id_type=MESH,
        )

    def sib_copy(h, zz, core):
        at = pl.ds(pl.multiple_of(((zz * HALVES + h) * 2 + core) * half, half), half)
        return pltpu.make_async_remote_copy(
            src_ref=gathered.at[at], dst_ref=gathered.at[at],
            send_sem=sib_send, recv_sem=sib_recv.at[zz * HALVES + h],
            device_id=(sib, chan), device_id_type=MESH,
        )

    def send_own(pieces):
        for h, turn in pieces:
            right, left = has_right, has_left
            if turn >= 2:
                right, left = jnp.logical_and(right, z != line - 2), jnp.logical_and(left, z != 1)
            pl.when(right)(line_copy(h, turn, z, me + SLAB).start)
            pl.when(left)(line_copy(h, turn, z, me - SLAB).start)

    order = [[(0, 0), (1, 0), (0, 1), (1, 1), (0, 2), (0, 3)], [(1, 2), (1, 3)]]
    for turn in range(SLAB):
        if turn:
            slab_wait(starts.at[quarter_rows(quarter_of(turn))], start_recv.at[turn - 1]).wait_recv()
        gate(z, q_ref, local, starts, quarter_of(turn) * quarter_blocks, quarter_blocks)
        if turn < 2:
            send_own(order[0][2 * turn:2 * turn + 2])
    pl.when(giver)(near_copies[2].start)
    send_own(order[0][4:] + order[1])
    for h in range(HALVES):
        sib_copy(h, z, c).start()
    loads[6].wait()

    def source(d, sign):
        zz = z - d if sign < 0 else z + d
        there = jnp.logical_and(zz >= 0, zz < line)
        if sign > 0:
            there = jnp.logical_and(there, d > 0)
        return zz, there

    def relay(d, h):
        taking = jnp.logical_and(taker, d == 1)
        for e, turn in order[h]:
            for sign in (-1, 1):
                zz, there = source(d, sign)
                if turn >= 2:
                    there = jnp.logical_and(there, jnp.logical_not(taking))

                @pl.when(there)
                def _():
                    line_copy(e, turn, zz, sib).wait_recv()
                    pl.when(has_right if sign < 0 else has_left)(line_copy(e, turn, zz, me - SLAB * sign).start)
                    if (e, turn) == order[h][-1]:
                        sib_copy(h, zz, c).start()

        if h == HALVES - 1:
            @pl.when(taking)
            def _():
                for copy in near_copies:
                    copy.wait_recv()
                gate(near, q_near, local_near, starts_near, (1 - x) * (blocks // 2), blocks // 2)
                for e in range(HALVES):
                    sib_copy(e, near, c).start()

    def relayless(sign):
        return z == 0 if sign > 0 else z + 2 >= line

    def compute(d, halves, other, part, side=None):
        for sign in (-1, 1):
            zz, there = source(d, sign)
            if side is not None:
                there = jnp.logical_and(there, relayless(sign) == side)

            @pl.when(there)
            def _():
                if not other:
                    for h in halves:
                        sib_copy(h, zz, 1 - c).wait_recv()
                size = 2 * half * len(halves)
                rows = pl.ds(pl.multiple_of((zz * HALVES + halves[0]) * 2 * half, 2 * half), size)
                at = pl.ds(part * cols, cols) if other else slice(None)
                weights = w_other if other else w_ref
                partial[other, rows, at] = jnp.dot(
                    gathered[rows], weights[:, at], preferred_element_type=F32
                ).astype(BF16)
                place = lax.rem(across if other else me, per_chan)
                for h in halves:
                    for core in range(2):
                        to = zz * SLAB + x * 2 + core
                        sent = pl.ds(pl.multiple_of(((zz * HALVES + h) * 2 + core) * half, half), half)
                        src = partial.at[other, sent, at]
                        if direct:
                            start = pl.multiple_of(place * width + part * cols, LANES)
                            dst = out_hbm.at[chan, pl.ds(h * half, half), pl.ds(start, cols if other else width)]
                        else:
                            dst = out_hbm.at[chan, place, pl.ds(h * half, half), at]
                        remote = pltpu.make_async_remote_copy(
                            src_ref=src, dst_ref=dst, send_sem=part_send, recv_sem=part_recv,
                            device_id=(to, out_chan), device_id_type=MESH,
                        )
                        here = pltpu.make_async_copy(src, dst, part_recv)
                        stays = jnp.logical_and(to == me, owner_plane)
                        pl.when(stays)(here.start)
                        pl.when(jnp.logical_not(stays))(remote.start)

    def each(first, last, body):
        def run(g, _):
            body(g)
            return 0

        lax.fori_loop(first, last, run, 0)

    last = line - 1
    split = 2
    whole = tuple(range(HALVES))


    for h in range(HALVES):
        relay(1, h)
    compute(0, whole, 0, 0)
    compute(1, whole, 0, 0, True)
    each(split, last, lambda d: relay(d, 0))
    swapped(0).wait_recv()
    compute(1, whole, 1, 0, True)
    compute(0, whole, 1, 0)
    each(split, last, lambda d: relay(d, 1))
    compute(1, whole, 0, 0, False)
    each(split, last, lambda d: compute(d, whole, 0, 0))
    compute(1, whole, 1, 0, False)
    each(split, last, lambda d: compute(d, whole, 1, 0))
    for h in range(HALVES):
        relay(last, h)
    for part in range(1, parts):
        swapped(part).wait_recv()
        each(0, last, lambda d: compute(last - 1 - d, whole, 1, part))
    compute(last, whole, 0, 0)
    for part in range(parts):
        compute(last, whole, 1, part)

    def drained(ref, sem):
        return pltpu.make_async_remote_copy(
            src_ref=ref, dst_ref=ref, send_sem=sem, recv_sem=sem, device_id=(sib, chan), device_id_type=MESH,
        )

    drained(out_hbm, part_recv).wait_recv()

    drained(ends_all.at[pl.ds(0, SLAB - 1)], end_send).wait_send()
    drained(starts_all.at[pl.ds(0, SLAB - 1)], start_send).wait_send()
    for hop in range(1, line):
        pl.when(z + hop < line)(carry_copy(hop).wait_send)
    for part in range(parts):
        swapped(part).wait_send()
    inner = jnp.logical_not(jnp.logical_or(taker, giver))
    pl.when(inner)(drained(gathered.at[pl.ds(0, (line + 1) * tok)], line_send).wait_send)
    pl.when(taker)(drained(gathered.at[pl.ds(0, tok)], line_send).wait_send)
    pl.when(giver)(drained(gathered.at[pl.ds(0, line * tok + tok // 2)], line_send).wait_send)
    for copy in near_copies:
        pl.when(giver)(copy.wait_send)
    drained(gathered.at[pl.ds(0, line * tok)], sib_send).wait_send()
    pl.when(owner_plane)(drained(partial.at[:, pl.ds(0, (2 * line - 1) * tok)], part_send).wait_send)
    pl.when(jnp.logical_not(owner_plane))(drained(partial, part_send).wait_send)


def solution(mesh):
    n, n_chan = mesh.shape["seq"], mesh.shape["chan"]
    assert n % (SLAB * n_chan) == 0 and n >= 4 * SLAB

    def body(gate_input, key_input, value_input, decay_rate, residue, skip_gain, out_weight):
        tok, chans = gate_input.shape
        modes = decay_rate.shape[0]
        width = out_weight.shape[1]
        line = n // SLAB
        quarter = modes * chans // (LANES * SLAB)
        rows = 2 * line * tok
        direct = width % LANES == 0
        hbm = pl.BlockSpec(memory_space=pltpu.HBM)
        dma = pltpu.SemaphoreType.DMA
        slab_states = pltpu.VMEM((SLAB, quarter, LANES), BF16)
        all_states = pltpu.VMEM((SLAB * quarter, LANES), BF16)
        per_chan = n // n_chan
        landing = (n_chan, tok, width * per_chan) if direct else (n_chan, per_chan, tok, width)
        landed = pl.pallas_call(
            functools.partial(kernel, n, n_chan),
            out_shape=jax.ShapeDtypeStruct(landing, BF16),
            in_specs=[hbm] * 7,
            out_specs=pl.BlockSpec(memory_space=pl.ANY),
            scratch_shapes=[
                pltpu.VMEM((tok, chans), BF16),
                pltpu.VMEM((tok, chans), BF16),
                pltpu.VMEM((tok, chans), BF16),
                pltpu.VMEM((modes, chans), F32),
                pltpu.VMEM((modes, chans), F32),
                pltpu.VMEM((1, chans), F32),
                pltpu.VMEM((chans, width), BF16),
                pltpu.VMEM((chans, width), BF16),
                dma((7,)), dma((column_parts(width),)), dma((column_parts(width),)),
                pltpu.VMEM((tok, chans), F32),
                pltpu.VMEM((tok, chans), F32),
                pltpu.VMEM((tok + SUB, LANES), F32),
                all_states, slab_states, pltpu.VMEM((line, quarter, LANES), BF16), pltpu.VMEM((quarter, LANES), BF16),
                slab_states, all_states,
                pltpu.VMEM((tok, chans), BF16), pltpu.VMEM((tok, chans), BF16), pltpu.VMEM((tok, chans), BF16), all_states,
                pltpu.VMEM((rows, chans), BF16),
                pltpu.VMEM((2, rows, width), BF16),
                pltpu.SemaphoreType.REGULAR, dma(()), dma(()), dma((line,)), dma((line,)), dma(()), dma((SLAB - 1,)),
                dma((3,)), dma((3,)), dma(()), dma((line * HALVES * SLAB,)), dma(()), dma((line * HALVES,)),
                dma(()), dma(()),
            ],
            compiler_params=pltpu.CompilerParams(
                collective_id=0, has_side_effects=True, vmem_limit_bytes=40 * 2**20
            ),
            cost_estimate=pl.CostEstimate(
                flops=2 * n * tok * chans * width, bytes_accessed=4 * tok * chans, transcendentals=0
            ),
        )(*[
            pltpu.with_memory_space_constraint(array, pltpu.HBM)
            for array in (
                gate_input, key_input, value_input, decay_rate, residue, skip_gain.reshape(1, chans), out_weight
            )
        ])
        mixed = landed[0].astype(F32)
        for j in range(1, n_chan):
            mixed = mixed + landed[j].astype(F32)
        mixed = mixed.astype(BF16)
        return mixed if direct else mixed.transpose(1, 0, 2).reshape(tok, width * per_chan)

    return jax.shard_map(
        body,
        mesh=mesh,
        in_specs=(
            P("seq", "chan"),
            P("seq", "chan"),
            P("seq", "chan"),
            P(None, "chan"),
            P(None, "chan"),
            P("chan"),
            P("chan", "seq"),
        ),
        out_specs=P("seq", "chan"),
        check_vma=False,
    )
```

```python
import functools

import jax
import jax.numpy as jnp
from jax import lax
from jax.experimental import pallas as pl
from jax.experimental.pallas import tpu as pltpu
from jax.sharding import PartitionSpec as P

MESH = pl.DeviceIdType.MESH
F32 = jnp.float32
BF16 = jnp.bfloat16
LANES = 128
SUB = 8
SLAB = 4
HALVES = 2


def one_minus_exp(y):
    series = jnp.ones_like(y)
    for order in range(10, 1, -1):
        series = 1.0 - y * (1.0 / order) * series
    return jnp.where(y < 0.4, y * series, 1.0 - jnp.exp(-y))


def column_parts(width):
    return 2 if width % (2 * LANES) == 0 else 1


def kernel(
    n, n_chan,
    q_hbm, k_hbm, v_hbm, rate_hbm, residue_hbm, skip_hbm, w_hbm, out_hbm,
    q_ref, k_ref, v_ref, rate_ref, amp_ref, skip_ref, w_ref, w_other, load_sem, w_send, w_recv,
    sig, local, padded, ends, ends_all, carry_in, carry_out, starts_all, starts,
    local_out, q_near, local_near, starts_near, gathered, partial,
    ready, end_send, end_recv, carry_send, carry_recv, start_send, start_recv,
    near_send, near_recv, line_send, line_recv, sib_send, sib_recv, part_send, part_recv,
):
    tok, chans = q_ref.shape
    first_loads = [
        [
            pltpu.make_async_copy(source.at[:, at], target.at[:, at], load_sem.at[7 + 3 * i + j])
            for j, (source, target) in enumerate([(k_hbm, k_ref), (v_hbm, v_ref), (rate_hbm, rate_ref)])
        ]
        for i, at in enumerate([pl.ds(0, chans // 2), pl.ds(chans // 2, chans // 2)])
    ]
    loads = [None] * 3 + [
        pltpu.make_async_copy(source, target, load_sem.at[3 + i])
        for i, (source, target) in enumerate([
            (residue_hbm, amp_ref), (skip_hbm, skip_ref), (q_hbm, q_ref), (w_hbm, w_ref),
        ])
    ]
    for load in first_loads[0] + first_loads[1] + loads[3:]:
        load.start()
    modes = rate_ref.shape[0]
    blocks = chans // LANES
    width = w_ref.shape[1]
    per_chan = n // n_chan
    line = n // SLAB
    tiles = tok // SUB
    quarter_blocks = blocks // SLAB
    quarter = quarter_blocks * modes
    half = tok // HALVES
    parts = column_parts(width)
    cols = width // parts
    direct = width % LANES == 0

    me = lax.axis_index("seq")
    chan = lax.axis_index("chan")
    z = me // SLAB
    x = (me // 2) % 2
    c = me % 2
    qd = me % SLAB
    sib = me + 1 - 2 * c
    across = me + 2 - 4 * x
    has_right = z < line - 1
    has_left = z > 0
    out_chan = me // per_chan
    owner_plane = chan == out_chan
    giver = jnp.logical_or(z == 1, z == line - 2)
    taker = jnp.logical_not(jnp.logical_and(has_left, has_right))
    near = jnp.where(z == 0, 1, line - 2)
    taken_by = jnp.where(z == 1, me - SLAB, me + SLAB)

    def quarter_of(turn):
        return (x if turn < 2 else 1 - x) * 2 + (c if turn % 2 == 0 else 1 - c)

    def mate(turn):
        return me - qd + quarter_of(turn)

    barrier = pltpu.get_barrier_semaphore()

    def hello(seq, ch):
        pl.semaphore_signal(barrier, inc=1, device_id=(seq, ch), device_id_type=MESH)

    for turn in range(1, SLAB):
        hello(mate(turn), chan)
    pl.when(has_right)(lambda: hello(me + SLAB, chan))
    pl.when(has_left)(lambda: hello(me - SLAB, chan))
    for turn in range(1, n_chan):
        hello(me, lax.rem(chan + turn, n_chan))
    greeters = SLAB - 1 + n_chan - 1 + has_right.astype(jnp.int32) + has_left.astype(jnp.int32)
    steps = lax.broadcasted_iota(jnp.int32, (SUB, LANES), 0).astype(F32)

    def lanes(b):
        return pl.ds(pl.multiple_of(b * LANES, LANES), LANES)

    def end_block(b, _):
        at = lanes(b)
        s = k_ref[:, at].astype(F32) * v_ref[:, at].astype(F32)
        sig[:, at] = s
        found = []
        for m in range(modes):
            rate = rate_ref[pl.ds(m, 1), at]
            jump = jnp.exp(-float(SUB) * rate)
            total = s[:SUB]
            for t in range(1, tiles):
                total = total * jump + s[t * SUB:(t + 1) * SUB]
            total = total * jnp.exp(-rate * (float(SUB - 1) - steps))
            found.append(jnp.sum(total, axis=0, keepdims=True))
        ends[pl.ds(pl.multiple_of(b * modes, modes), modes)] = jnp.concatenate(found, axis=0).astype(BF16)
        return 0

    for i in range(2):
        for load in first_loads[i]:
            load.wait()
        lax.fori_loop(i * blocks // 2, (i + 1) * blocks // 2, end_block, 0)

    pl.semaphore_wait(barrier, greeters)

    def quarter_rows(p):
        return pl.ds(pl.multiple_of(p * quarter, quarter), quarter)

    def slab_copy(source, target, send_sem, recv_sem, turn):
        return pltpu.make_async_remote_copy(
            src_ref=source, dst_ref=target, send_sem=send_sem, recv_sem=recv_sem,
            device_id=(mate(turn), chan), device_id_type=MESH,
        )

    def slab_wait(ref, sem):
        return slab_copy(ref, ref, sem, sem, 1)

    for turn in (2, 3, 1):
        slab_copy(ends.at[quarter_rows(quarter_of(turn))], ends_all.at[qd], end_send, end_recv, turn).start()
    ends_all[qd] = ends[quarter_rows(qd)]

    def near_copy(source, target, kind):
        return pltpu.make_async_remote_copy(
            src_ref=source, dst_ref=target, send_sem=near_send.at[kind], recv_sem=near_recv.at[kind],
            device_id=(taken_by, chan), device_id_type=MESH,
        )

    late_cols = pl.ds(pl.multiple_of((1 - x) * (chans // 2), chans // 2), chans // 2)
    late_states = pl.ds(pl.multiple_of((1 - x) * 2 * quarter, 2 * quarter), 2 * quarter)
    near_copies = [
        near_copy(q_hbm.at[:, late_cols], q_near.at[:, late_cols], 0),
        near_copy(local_out.at[:, late_cols], local_near.at[:, late_cols], 1),
        near_copy(starts.at[late_states], starts_near.at[late_states], 2),
    ]
    pl.when(giver)(near_copies[0].start)

    def swap(part, first, rows):
        at = (pl.ds(first, rows), pl.ds(part * cols, cols))
        pltpu.make_async_remote_copy(
            src_ref=w_hbm.at[at], dst_ref=w_other.at[at],
            send_sem=w_send.at[part], recv_sem=w_recv.at[part],
            device_id=(across, chan), device_id_type=MESH,
        ).start()

    def swapped(part):
        at = (slice(None), pl.ds(part * cols, cols))
        return pltpu.make_async_remote_copy(
            src_ref=w_other.at[at], dst_ref=w_other.at[at],
            send_sem=w_send.at[part], recv_sem=w_recv.at[part],
            device_id=(across, chan), device_id_type=MESH,
        )

    block_rows = LANES // 4
    middle_rows = chans * 7 // 32

    loads[3].wait()
    loads[4].wait()
    amp_ref[...] = amp_ref[...] * jnp.sqrt(one_minus_exp(2.0 * rate_ref[...]))

    padded[:SUB] = jnp.zeros((SUB, LANES), F32)

    def local_block(b, _):
        swap(0, pl.multiple_of(b * block_rows, block_rows), block_rows)
        at = lanes(b)
        response = [jnp.zeros((SUB, LANES), F32)] * tiles
        for m in range(modes):
            rate = rate_ref[pl.ds(m, 1), at]
            jump = jnp.exp(-float(SUB) * rate)
            term = amp_ref[pl.ds(m, 1), at] * jnp.exp(-rate * steps)
            for t in range(tiles):
                response[t] = response[t] + term
                if t < tiles - 1:
                    term = term * jump
        padded[SUB:] = jnp.concatenate(response, axis=0)
        skip = skip_ref[:, at]
        totals = [skip * sig[t * SUB:(t + 1) * SUB, at] for t in range(tiles)]
        for lag in range(SUB):
            moved = [padded[pl.ds(SUB - lag + t * SUB, SUB)] for t in range(tiles)]
            for first in range(tiles):
                value = sig[pl.ds(first * SUB + lag, 1), at]
                for t in range(first, tiles):
                    totals[t] = totals[t] + moved[t - first] * value
        totals = jnp.concatenate(totals, axis=0)
        local[:, at] = totals
        local_out[:, at] = totals.astype(BF16)
        return 0

    lax.fori_loop(0, blocks, local_block, 0)

    def signal_left():
        pl.semaphore_signal(ready, inc=1, device_id=(me - SLAB, chan), device_id_type=MESH)

    pl.when(z < line - 2)(lambda: pl.semaphore_wait(ready, 1))
    pl.when(jnp.logical_and(has_left, has_right))(signal_left)

    fades = jnp.concatenate(
        [jnp.exp(-float(tok) * rate_ref[:, lanes(qd * quarter_blocks + j)]) for j in range(quarter_blocks)], axis=0
    )
    slab_wait(ends_all.at[pl.ds(0, SLAB - 1)], end_recv).wait_recv()
    found = [ends_all[p].astype(F32) for p in range(SLAB)]
    slab_total = found[0]
    for p in range(1, SLAB):
        slab_total = slab_total * fades + found[p]
    slab_fade = (fades * fades) * (fades * fades)

    def carry_copy(hop):
        return pltpu.make_async_remote_copy(
            src_ref=carry_out, dst_ref=carry_in.at[z], send_sem=carry_send.at[hop - 1], recv_sem=carry_recv.at[z],
            device_id=(me + hop * SLAB, chan), device_id_type=MESH,
        )

    @pl.when(has_right)
    def _():
        carry_out[...] = slab_total.astype(BF16)
        for hop in range(1, line):
            pl.when(z + hop < line)(carry_copy(hop).start)

    pl.when(giver)(near_copies[1].start)

    @pl.when(has_left)
    def _():
        swap(0, blocks * block_rows, middle_rows)

    def collect(i, carry):
        pltpu.make_async_remote_copy(
            src_ref=carry_in.at[i], dst_ref=carry_in.at[i], send_sem=carry_send.at[0], recv_sem=carry_recv.at[i],
            device_id=(sib, chan), device_id_type=MESH,
        ).wait_recv()
        return carry * slab_fade + carry_in[i].astype(F32)

    carry = lax.fori_loop(0, z, collect, jnp.zeros((quarter, LANES), F32))

    state = carry
    for p in range(SLAB):
        starts_all[p] = state.astype(BF16)
        if p < SLAB - 1:
            state = state * fades + found[p]
    for turn in (2, 3, 1):
        slab_copy(
            starts_all.at[quarter_of(turn)], starts.at[quarter_rows(qd)], start_send, start_recv.at[turn - 1], turn
        ).start()
    starts[quarter_rows(qd)] = starts_all[qd]

    @pl.when(jnp.logical_not(has_left))
    def _():
        swap(0, blocks * block_rows, middle_rows)

    swap(0, blocks * block_rows + middle_rows, chans - blocks * block_rows - middle_rows)
    for part in range(1, parts):
        swap(part, 0, chans)
    loads[5].wait()

    def gate(zz, q_from, local_from, starts_from, first, count):
        targets = [
            pl.ds(pl.multiple_of(((zz * HALVES + h) * 2 + c) * half, half), half) for h in range(HALVES)
        ]

        def gate_block(b, _):
            at = lanes(b)
            held = starts_from[pl.ds(pl.multiple_of(b * modes, modes), modes)].astype(F32)
            found = local_from[:, at].astype(F32)
            totals = [found[t * SUB:(t + 1) * SUB] for t in range(tiles)]
            for m in range(modes):
                rate = rate_ref[pl.ds(m, 1), at]
                jump = jnp.exp(-float(SUB) * rate)
                term = (amp_ref[pl.ds(m, 1), at] * held[m:m + 1]) * jnp.exp(-rate * (steps + 1.0))
                for t in range(tiles):
                    totals[t] = totals[t] + term
                    if t < tiles - 1:
                        term = term * jump
            gated = (q_from[:, at].astype(F32) * jnp.concatenate(totals, axis=0)).astype(BF16)
            for h in range(HALVES):
                gathered[targets[h], at] = gated[h * half:(h + 1) * half]
            return 0

        lax.fori_loop(first, first + count, gate_block, 0)

    quarter_cols = chans // SLAB

    def line_copy(h, turn, zz, peer):
        at = (
            pl.ds(pl.multiple_of(((zz * HALVES + h) * 2 + c) * half, half), half),
            pl.ds(pl.multiple_of(quarter_of(turn) * quarter_cols, quarter_cols), quarter_cols),
        )
        return pltpu.make_async_remote_copy(
            src_ref=gathered.at[at], dst_ref=gathered.at[at],
            send_sem=line_send, recv_sem=line_recv.at[(zz * HALVES + h) * SLAB + turn],
            device_id=(peer, chan), device_id_type=MESH,
        )

    def sib_copy(h, zz, core):
        at = pl.ds(pl.multiple_of(((zz * HALVES + h) * 2 + core) * half, half), half)
        return pltpu.make_async_remote_copy(
            src_ref=gathered.at[at], dst_ref=gathered.at[at],
            send_sem=sib_send, recv_sem=sib_recv.at[zz * HALVES + h],
            device_id=(sib, chan), device_id_type=MESH,
        )

    def send_own(pieces):
        for h, turn in pieces:
            right, left = has_right, has_left
            if turn >= 2:
                right, left = jnp.logical_and(right, z != line - 2), jnp.logical_and(left, z != 1)
            pl.when(right)(line_copy(h, turn, z, me + SLAB).start)
            pl.when(left)(line_copy(h, turn, z, me - SLAB).start)

    order = [[(0, 0), (1, 0), (0, 1), (1, 1), (0, 2), (0, 3)], [(1, 2), (1, 3)]]
    for turn in range(SLAB):
        if turn:
            slab_wait(starts.at[quarter_rows(quarter_of(turn))], start_recv.at[turn - 1]).wait_recv()
        gate(z, q_ref, local, starts, quarter_of(turn) * quarter_blocks, quarter_blocks)
        if turn < 2:
            send_own(order[0][2 * turn:2 * turn + 2])
    pl.when(giver)(near_copies[2].start)
    send_own(order[0][4:] + order[1])
    for h in range(HALVES):
        sib_copy(h, z, c).start()
    loads[6].wait()

    def source(d, sign):
        zz = z - d if sign < 0 else z + d
        there = jnp.logical_and(zz >= 0, zz < line)
        if sign > 0:
            there = jnp.logical_and(there, d > 0)
        return zz, there

    def relay(d, h):
        taking = jnp.logical_and(taker, d == 1)
        for e, turn in order[h]:
            for sign in (-1, 1):
                zz, there = source(d, sign)
                if turn >= 2:
                    there = jnp.logical_and(there, jnp.logical_not(taking))

                @pl.when(there)
                def _():
                    line_copy(e, turn, zz, sib).wait_recv()
                    pl.when(has_right if sign < 0 else has_left)(line_copy(e, turn, zz, me - SLAB * sign).start)
                    if (e, turn) == order[h][-1]:
                        sib_copy(h, zz, c).start()

        if h == HALVES - 1:
            @pl.when(taking)
            def _():
                for copy in near_copies:
                    copy.wait_recv()
                gate(near, q_near, local_near, starts_near, (1 - x) * (blocks // 2), blocks // 2)
                for e in range(HALVES):
                    sib_copy(e, near, c).start()

    def relayless(sign):
        return z == 0 if sign > 0 else z + 2 >= line

    def compute(d, halves, other, part, side=None):
        for sign in (-1, 1):
            zz, there = source(d, sign)
            if side is not None:
                there = jnp.logical_and(there, relayless(sign) == side)

            @pl.when(there)
            def _():
                if not other:
                    for h in halves:
                        sib_copy(h, zz, 1 - c).wait_recv()
                size = 2 * half * len(halves)
                rows = pl.ds(pl.multiple_of((zz * HALVES + halves[0]) * 2 * half, 2 * half), size)
                at = pl.ds(part * cols, cols) if other else slice(None)
                weights = w_other if other else w_ref
                partial[other, rows, at] = jnp.dot(
                    gathered[rows], weights[:, at], preferred_element_type=F32
                ).astype(BF16)
                place = lax.rem(across if other else me, per_chan)
                for h in halves:
                    for core in range(2):
                        to = zz * SLAB + x * 2 + core
                        sent = pl.ds(pl.multiple_of(((zz * HALVES + h) * 2 + core) * half, half), half)
                        src = partial.at[other, sent, at]
                        if direct:
                            start = pl.multiple_of(place * width + part * cols, LANES)
                            dst = out_hbm.at[chan, pl.ds(h * half, half), pl.ds(start, cols if other else width)]
                        else:
                            dst = out_hbm.at[chan, place, pl.ds(h * half, half), at]
                        remote = pltpu.make_async_remote_copy(
                            src_ref=src, dst_ref=dst, send_sem=part_send, recv_sem=part_recv,
                            device_id=(to, out_chan), device_id_type=MESH,
                        )
                        here = pltpu.make_async_copy(src, dst, part_recv)
                        stays = jnp.logical_and(to == me, owner_plane)
                        pl.when(stays)(here.start)
                        pl.when(jnp.logical_not(stays))(remote.start)

    def each(first, last, body):
        def run(g, _):
            body(g)
            return 0

        lax.fori_loop(first, last, run, 0)

    last = line - 1
    split = 2
    whole = tuple(range(HALVES))


    for h in range(HALVES):
        relay(1, h)
    compute(0, whole, 0, 0)
    compute(1, whole, 0, 0, True)
    each(split, last, lambda d: relay(d, 0))
    swapped(0).wait_recv()
    compute(1, whole, 1, 0, True)
    compute(0, whole, 1, 0)
    each(split, last, lambda d: relay(d, 1))
    compute(1, whole, 0, 0, False)
    each(split, last, lambda d: compute(d, whole, 0, 0))
    compute(1, whole, 1, 0, False)
    each(split, last, lambda d: compute(d, whole, 1, 0))
    for h in range(HALVES):
        relay(last, h)
    for part in range(1, parts):
        swapped(part).wait_recv()
        each(0, last, lambda d: compute(d, whole, 1, part))
    for h in range(HALVES):
        compute(last, (h,), 0, 0)
    for part in range(parts):
        compute(last, whole, 1, part)

    def drained(ref, sem):
        return pltpu.make_async_remote_copy(
            src_ref=ref, dst_ref=ref, send_sem=sem, recv_sem=sem, device_id=(sib, chan), device_id_type=MESH,
        )

    drained(out_hbm, part_recv).wait_recv()

    drained(ends_all.at[pl.ds(0, SLAB - 1)], end_send).wait_send()
    drained(starts_all.at[pl.ds(0, SLAB - 1)], start_send).wait_send()
    for hop in range(1, line):
        pl.when(z + hop < line)(carry_copy(hop).wait_send)
    for part in range(parts):
        swapped(part).wait_send()
    inner = jnp.logical_not(jnp.logical_or(taker, giver))
    pl.when(inner)(drained(gathered.at[pl.ds(0, (line + 1) * tok)], line_send).wait_send)
    pl.when(taker)(drained(gathered.at[pl.ds(0, tok)], line_send).wait_send)
    pl.when(giver)(drained(gathered.at[pl.ds(0, line * tok + tok // 2)], line_send).wait_send)
    for copy in near_copies:
        pl.when(giver)(copy.wait_send)
    drained(gathered.at[pl.ds(0, line * tok)], sib_send).wait_send()
    pl.when(owner_plane)(drained(partial.at[:, pl.ds(0, (2 * line - 1) * tok)], part_send).wait_send)
    pl.when(jnp.logical_not(owner_plane))(drained(partial, part_send).wait_send)


def solution(mesh):
    n, n_chan = mesh.shape["seq"], mesh.shape["chan"]
    assert n % (SLAB * n_chan) == 0 and n >= 4 * SLAB

    def body(gate_input, key_input, value_input, decay_rate, residue, skip_gain, out_weight):
        tok, chans = gate_input.shape
        modes = decay_rate.shape[0]
        width = out_weight.shape[1]
        line = n // SLAB
        quarter = modes * chans // (LANES * SLAB)
        rows = 2 * line * tok
        direct = width % LANES == 0
        hbm = pl.BlockSpec(memory_space=pltpu.HBM)
        dma = pltpu.SemaphoreType.DMA
        slab_states = pltpu.VMEM((SLAB, quarter, LANES), BF16)
        all_states = pltpu.VMEM((SLAB * quarter, LANES), BF16)
        per_chan = n // n_chan
        landing = (n_chan, tok, width * per_chan) if direct else (n_chan, per_chan, tok, width)
        landed = pl.pallas_call(
            functools.partial(kernel, n, n_chan),
            out_shape=jax.ShapeDtypeStruct(landing, BF16),
            in_specs=[hbm] * 7,
            out_specs=pl.BlockSpec(memory_space=pl.ANY),
            scratch_shapes=[
                pltpu.VMEM((tok, chans), BF16),
                pltpu.VMEM((tok, chans), BF16),
                pltpu.VMEM((tok, chans), BF16),
                pltpu.VMEM((modes, chans), F32),
                pltpu.VMEM((modes, chans), F32),
                pltpu.VMEM((1, chans), F32),
                pltpu.VMEM((chans, width), BF16),
                pltpu.VMEM((chans, width), BF16),
                dma((13,)), dma((column_parts(width),)), dma((column_parts(width),)),
                pltpu.VMEM((tok, chans), F32),
                pltpu.VMEM((tok, chans), F32),
                pltpu.VMEM((tok + SUB, LANES), F32),
                all_states, slab_states, pltpu.VMEM((line, quarter, LANES), BF16), pltpu.VMEM((quarter, LANES), BF16),
                slab_states, all_states,
                pltpu.VMEM((tok, chans), BF16), pltpu.VMEM((tok, chans), BF16), pltpu.VMEM((tok, chans), BF16), all_states,
                pltpu.VMEM((rows, chans), BF16),
                pltpu.VMEM((2, rows, width), BF16),
                pltpu.SemaphoreType.REGULAR, dma(()), dma(()), dma((line,)), dma((line,)), dma(()), dma((SLAB - 1,)),
                dma((3,)), dma((3,)), dma(()), dma((line * HALVES * SLAB,)), dma(()), dma((line * HALVES,)),
                dma(()), dma(()),
            ],
            compiler_params=pltpu.CompilerParams(
                collective_id=0, has_side_effects=True, vmem_limit_bytes=40 * 2**20
            ),
            cost_estimate=pl.CostEstimate(
                flops=2 * n * tok * chans * width, bytes_accessed=4 * tok * chans, transcendentals=0
            ),
        )(*[
            pltpu.with_memory_space_constraint(array, pltpu.HBM)
            for array in (
                gate_input, key_input, value_input, decay_rate, residue, skip_gain.reshape(1, chans), out_weight
            )
        ])
        mixed = landed[0].astype(F32)
        for j in range(1, n_chan):
            mixed = mixed + landed[j].astype(F32)
        mixed = mixed.astype(BF16)
        return mixed if direct else mixed.transpose(1, 0, 2).reshape(tok, width * per_chan)

    return jax.shard_map(
        body,
        mesh=mesh,
        in_specs=(
            P("seq", "chan"),
            P("seq", "chan"),
            P("seq", "chan"),
            P(None, "chan"),
            P(None, "chan"),
            P("chan"),
            P("chan", "seq"),
        ),
        out_specs=P("seq", "chan"),
        check_vma=False,
    )
```

```python
import functools

import jax
import jax.numpy as jnp
from jax import lax
from jax.experimental import pallas as pl
from jax.experimental.pallas import tpu as pltpu
from jax.sharding import PartitionSpec as P

MESH = pl.DeviceIdType.MESH
F32 = jnp.float32
BF16 = jnp.bfloat16
LANES = 128
SUB = 8
SLAB = 4
HALVES = 2


def one_minus_exp(y):
    series = jnp.ones_like(y)
    for order in range(10, 1, -1):
        series = 1.0 - y * (1.0 / order) * series
    return jnp.where(y < 0.4, y * series, 1.0 - jnp.exp(-y))


def column_parts(width):
    return 2 if width % (2 * LANES) == 0 else 1


def kernel(
    n, n_chan,
    q_hbm, k_hbm, v_hbm, rate_hbm, residue_hbm, skip_hbm, w_hbm, out_hbm,
    q_ref, k_ref, v_ref, rate_ref, amp_ref, skip_ref, w_ref, w_other, load_sem, w_send, w_recv,
    sig, local, padded, ends, ends_all, carry_in, carry_out, starts_all, starts,
    local_out, q_near, local_near, starts_near, gathered, partial,
    ready, end_send, end_recv, carry_send, carry_recv, start_send, start_recv,
    near_send, near_recv, line_send, line_recv, sib_send, sib_recv, part_send, part_recv,
):
    tok, chans = q_ref.shape
    first_loads = [
        [
            pltpu.make_async_copy(source.at[:, at], target.at[:, at], load_sem.at[7 + 3 * i + j])
            for j, (source, target) in enumerate([(k_hbm, k_ref), (v_hbm, v_ref), (rate_hbm, rate_ref)])
        ]
        for i, at in enumerate([pl.ds(0, chans // 2), pl.ds(chans // 2, chans // 2)])
    ]
    loads = [None] * 3 + [
        pltpu.make_async_copy(source, target, load_sem.at[3 + i])
        for i, (source, target) in enumerate([
            (residue_hbm, amp_ref), (skip_hbm, skip_ref), (q_hbm, q_ref), (w_hbm, w_ref),
        ])
    ]
    for load in first_loads[0] + first_loads[1] + loads[3:]:
        load.start()
    modes = rate_ref.shape[0]
    blocks = chans // LANES
    width = w_ref.shape[1]
    per_chan = n // n_chan
    line = n // SLAB
    tiles = tok // SUB
    quarter_blocks = blocks // SLAB
    quarter = quarter_blocks * modes
    half = tok // HALVES
    parts = column_parts(width)
    cols = width // parts
    direct = width % LANES == 0

    me = lax.axis_index("seq")
    chan = lax.axis_index("chan")
    z = me // SLAB
    x = (me // 2) % 2
    c = me % 2
    qd = me % SLAB
    sib = me + 1 - 2 * c
    across = me + 2 - 4 * x
    has_right = z < line - 1
    has_left = z > 0
    out_chan = me // per_chan
    owner_plane = chan == out_chan
    giver = jnp.logical_or(z == 1, z == line - 2)
    taker = jnp.logical_not(jnp.logical_and(has_left, has_right))
    near = jnp.where(z == 0, 1, line - 2)
    taken_by = jnp.where(z == 1, me - SLAB, me + SLAB)

    def quarter_of(turn):
        return (x if turn < 2 else 1 - x) * 2 + (c if turn % 2 == 0 else 1 - c)

    def mate(turn):
        return me - qd + quarter_of(turn)

    barrier = pltpu.get_barrier_semaphore()

    def hello(seq, ch):
        pl.semaphore_signal(barrier, inc=1, device_id=(seq, ch), device_id_type=MESH)

    for turn in range(1, SLAB):
        hello(mate(turn), chan)
    pl.when(has_right)(lambda: hello(me + SLAB, chan))
    pl.when(has_left)(lambda: hello(me - SLAB, chan))
    for turn in range(1, n_chan):
        hello(me, lax.rem(chan + turn, n_chan))
    greeters = SLAB - 1 + n_chan - 1 + has_right.astype(jnp.int32) + has_left.astype(jnp.int32)
    steps = lax.broadcasted_iota(jnp.int32, (SUB, LANES), 0).astype(F32)

    def lanes(b):
        return pl.ds(pl.multiple_of(b * LANES, LANES), LANES)

    def end_block(b, _):
        at = lanes(b)
        s = k_ref[:, at].astype(F32) * v_ref[:, at].astype(F32)
        sig[:, at] = s
        found = []
        for m in range(modes):
            rate = rate_ref[pl.ds(m, 1), at]
            jump = jnp.exp(-float(SUB) * rate)
            total = s[:SUB]
            for t in range(1, tiles):
                total = total * jump + s[t * SUB:(t + 1) * SUB]
            total = total * jnp.exp(-rate * (float(SUB - 1) - steps))
            found.append(jnp.sum(total, axis=0, keepdims=True))
        ends[pl.ds(pl.multiple_of(b * modes, modes), modes)] = jnp.concatenate(found, axis=0).astype(BF16)
        return 0

    for i in range(2):
        for load in first_loads[i]:
            load.wait()
        lax.fori_loop(i * blocks // 2, (i + 1) * blocks // 2, end_block, 0)

    pl.semaphore_wait(barrier, greeters)

    def quarter_rows(p):
        return pl.ds(pl.multiple_of(p * quarter, quarter), quarter)

    def slab_copy(source, target, send_sem, recv_sem, turn):
        return pltpu.make_async_remote_copy(
            src_ref=source, dst_ref=target, send_sem=send_sem, recv_sem=recv_sem,
            device_id=(mate(turn), chan), device_id_type=MESH,
        )

    def slab_wait(ref, sem):
        return slab_copy(ref, ref, sem, sem, 1)

    for turn in (2, 3, 1):
        slab_copy(ends.at[quarter_rows(quarter_of(turn))], ends_all.at[qd], end_send, end_recv, turn).start()
    ends_all[qd] = ends[quarter_rows(qd)]

    def near_copy(source, target, kind):
        return pltpu.make_async_remote_copy(
            src_ref=source, dst_ref=target, send_sem=near_send.at[kind], recv_sem=near_recv.at[kind],
            device_id=(taken_by, chan), device_id_type=MESH,
        )

    late_cols = pl.ds(pl.multiple_of((1 - x) * (chans // 2), chans // 2), chans // 2)
    late_states = pl.ds(pl.multiple_of((1 - x) * 2 * quarter, 2 * quarter), 2 * quarter)
    near_copies = [
        near_copy(q_hbm.at[:, late_cols], q_near.at[:, late_cols], 0),
        near_copy(local_out.at[:, late_cols], local_near.at[:, late_cols], 1),
        near_copy(starts.at[late_states], starts_near.at[late_states], 2),
    ]
    pl.when(giver)(near_copies[0].start)

    def swap(part, first, rows):
        at = (pl.ds(first, rows), pl.ds(part * cols, cols))
        pltpu.make_async_remote_copy(
            src_ref=w_hbm.at[at], dst_ref=w_other.at[at],
            send_sem=w_send.at[part], recv_sem=w_recv.at[part],
            device_id=(across, chan), device_id_type=MESH,
        ).start()

    def swapped(part):
        at = (slice(None), pl.ds(part * cols, cols))
        return pltpu.make_async_remote_copy(
            src_ref=w_other.at[at], dst_ref=w_other.at[at],
            send_sem=w_send.at[part], recv_sem=w_recv.at[part],
            device_id=(across, chan), device_id_type=MESH,
        )

    block_rows = LANES // 4
    middle_rows = chans * 7 // 32

    loads[3].wait()
    loads[4].wait()
    amp_ref[...] = amp_ref[...] * jnp.sqrt(one_minus_exp(2.0 * rate_ref[...]))

    padded[:SUB] = jnp.zeros((SUB, LANES), F32)

    def local_block(b, _):
        swap(0, pl.multiple_of(b * block_rows, block_rows), block_rows)
        at = lanes(b)
        response = [jnp.zeros((SUB, LANES), F32)] * tiles
        for m in range(modes):
            rate = rate_ref[pl.ds(m, 1), at]
            jump = jnp.exp(-float(SUB) * rate)
            term = amp_ref[pl.ds(m, 1), at] * jnp.exp(-rate * steps)
            for t in range(tiles):
                response[t] = response[t] + term
                if t < tiles - 1:
                    term = term * jump
        padded[SUB:] = jnp.concatenate(response, axis=0)
        skip = skip_ref[:, at]
        totals = [skip * sig[t * SUB:(t + 1) * SUB, at] for t in range(tiles)]
        for lag in range(SUB):
            moved = [padded[pl.ds(SUB - lag + t * SUB, SUB)] for t in range(tiles)]
            for first in range(tiles):
                value = sig[pl.ds(first * SUB + lag, 1), at]
                for t in range(first, tiles):
                    totals[t] = totals[t] + moved[t - first] * value
        totals = jnp.concatenate(totals, axis=0)
        local[:, at] = totals
        local_out[:, at] = totals.astype(BF16)
        return 0

    lax.fori_loop(0, blocks, local_block, 0)

    def signal_left():
        pl.semaphore_signal(ready, inc=1, device_id=(me - SLAB, chan), device_id_type=MESH)

    pl.when(z < line - 2)(lambda: pl.semaphore_wait(ready, 1))
    pl.when(jnp.logical_and(has_left, has_right))(signal_left)

    fades = jnp.concatenate(
        [jnp.exp(-float(tok) * rate_ref[:, lanes(qd * quarter_blocks + j)]) for j in range(quarter_blocks)], axis=0
    )
    slab_wait(ends_all.at[pl.ds(0, SLAB - 1)], end_recv).wait_recv()
    found = [ends_all[p].astype(F32) for p in range(SLAB)]
    slab_total = found[0]
    for p in range(1, SLAB):
        slab_total = slab_total * fades + found[p]
    slab_fade = (fades * fades) * (fades * fades)

    def carry_copy(hop):
        return pltpu.make_async_remote_copy(
            src_ref=carry_out, dst_ref=carry_in.at[z], send_sem=carry_send.at[hop - 1], recv_sem=carry_recv.at[z],
            device_id=(me + hop * SLAB, chan), device_id_type=MESH,
        )

    @pl.when(has_right)
    def _():
        carry_out[...] = slab_total.astype(BF16)
        for hop in range(1, line):
            pl.when(z + hop < line)(carry_copy(hop).start)

    pl.when(giver)(near_copies[1].start)

    @pl.when(has_left)
    def _():
        swap(0, blocks * block_rows, middle_rows)

    def collect(i, carry):
        pltpu.make_async_remote_copy(
            src_ref=carry_in.at[i], dst_ref=carry_in.at[i], send_sem=carry_send.at[0], recv_sem=carry_recv.at[i],
            device_id=(sib, chan), device_id_type=MESH,
        ).wait_recv()
        return carry * slab_fade + carry_in[i].astype(F32)

    carry = lax.fori_loop(0, z, collect, jnp.zeros((quarter, LANES), F32))

    state = carry
    for p in range(SLAB):
        starts_all[p] = state.astype(BF16)
        if p < SLAB - 1:
            state = state * fades + found[p]
    for turn in (2, 3, 1):
        slab_copy(
            starts_all.at[quarter_of(turn)], starts.at[quarter_rows(qd)], start_send, start_recv.at[turn - 1], turn
        ).start()
    starts[quarter_rows(qd)] = starts_all[qd]

    @pl.when(jnp.logical_not(has_left))
    def _():
        swap(0, blocks * block_rows, middle_rows)

    swap(0, blocks * block_rows + middle_rows, chans - blocks * block_rows - middle_rows)
    for part in range(1, parts):
        swap(part, 0, chans)
    loads[5].wait()

    def gate(zz, q_from, local_from, starts_from, first, count):
        targets = [
            pl.ds(pl.multiple_of(((zz * HALVES + h) * 2 + c) * half, half), half) for h in range(HALVES)
        ]

        def gate_block(b, _):
            at = lanes(b)
            held = starts_from[pl.ds(pl.multiple_of(b * modes, modes), modes)].astype(F32)
            found = local_from[:, at].astype(F32)
            totals = [found[t * SUB:(t + 1) * SUB] for t in range(tiles)]
            for m in range(modes):
                rate = rate_ref[pl.ds(m, 1), at]
                jump = jnp.exp(-float(SUB) * rate)
                term = (amp_ref[pl.ds(m, 1), at] * held[m:m + 1]) * jnp.exp(-rate * (steps + 1.0))
                for t in range(tiles):
                    totals[t] = totals[t] + term
                    if t < tiles - 1:
                        term = term * jump
            gated = (q_from[:, at].astype(F32) * jnp.concatenate(totals, axis=0)).astype(BF16)
            for h in range(HALVES):
                gathered[targets[h], at] = gated[h * half:(h + 1) * half]
            return 0

        lax.fori_loop(first, first + count, gate_block, 0)

    quarter_cols = chans // SLAB

    def line_copy(h, turn, zz, peer):
        at = (
            pl.ds(pl.multiple_of(((zz * HALVES + h) * 2 + c) * half, half), half),
            pl.ds(pl.multiple_of(quarter_of(turn) * quarter_cols, quarter_cols), quarter_cols),
        )
        return pltpu.make_async_remote_copy(
            src_ref=gathered.at[at], dst_ref=gathered.at[at],
            send_sem=line_send, recv_sem=line_recv.at[(zz * HALVES + h) * SLAB + turn],
            device_id=(peer, chan), device_id_type=MESH,
        )

    def sib_copy(h, zz, core):
        at = pl.ds(pl.multiple_of(((zz * HALVES + h) * 2 + core) * half, half), half)
        return pltpu.make_async_remote_copy(
            src_ref=gathered.at[at], dst_ref=gathered.at[at],
            send_sem=sib_send, recv_sem=sib_recv.at[zz * HALVES + h],
            device_id=(sib, chan), device_id_type=MESH,
        )

    def send_own(pieces):
        for h, turn in pieces:
            right, left = has_right, has_left
            if turn >= 2:
                right, left = jnp.logical_and(right, z != line - 2), jnp.logical_and(left, z != 1)
            pl.when(right)(line_copy(h, turn, z, me + SLAB).start)
            pl.when(left)(line_copy(h, turn, z, me - SLAB).start)

    order = [[(0, 0), (1, 0), (0, 1), (1, 1), (0, 2), (1, 2), (0, 3)], [(1, 3)]]
    for turn in range(SLAB):
        if turn:
            slab_wait(starts.at[quarter_rows(quarter_of(turn))], start_recv.at[turn - 1]).wait_recv()
        gate(z, q_ref, local, starts, quarter_of(turn) * quarter_blocks, quarter_blocks)
        if turn < SLAB - 1:
            send_own(order[0][2 * turn:2 * turn + 2])
    pl.when(giver)(near_copies[2].start)
    send_own(order[0][6:] + order[1])
    for h in range(HALVES):
        sib_copy(h, z, c).start()
    loads[6].wait()

    def source(d, sign):
        zz = z - d if sign < 0 else z + d
        there = jnp.logical_and(zz >= 0, zz < line)
        if sign > 0:
            there = jnp.logical_and(there, d > 0)
        return zz, there

    def relay(d, h):
        taking = jnp.logical_and(taker, d == 1)
        for e, turn in order[h]:
            for sign in (-1, 1):
                zz, there = source(d, sign)
                if turn >= 2:
                    there = jnp.logical_and(there, jnp.logical_not(taking))

                @pl.when(there)
                def _():
                    line_copy(e, turn, zz, sib).wait_recv()
                    pl.when(has_right if sign < 0 else has_left)(line_copy(e, turn, zz, me - SLAB * sign).start)
                    if (e, turn) == order[h][-1]:
                        sib_copy(h, zz, c).start()

        if h == HALVES - 1:
            @pl.when(taking)
            def _():
                for copy in near_copies:
                    copy.wait_recv()
                gate(near, q_near, local_near, starts_near, (1 - x) * (blocks // 2), blocks // 2)
                for e in range(HALVES):
                    sib_copy(e, near, c).start()

    def relayless(sign):
        return z == 0 if sign > 0 else z + 2 >= line

    def compute(d, halves, other, part, side=None):
        for sign in (-1, 1):
            zz, there = source(d, sign)
            if side is not None:
                there = jnp.logical_and(there, relayless(sign) == side)

            @pl.when(there)
            def _():
                if not other:
                    for h in halves:
                        sib_copy(h, zz, 1 - c).wait_recv()
                size = 2 * half * len(halves)
                rows = pl.ds(pl.multiple_of((zz * HALVES + halves[0]) * 2 * half, 2 * half), size)
                at = pl.ds(part * cols, cols) if other else slice(None)
                weights = w_other if other else w_ref
                partial[other, rows, at] = jnp.dot(
                    gathered[rows], weights[:, at], preferred_element_type=F32
                ).astype(BF16)
                place = lax.rem(across if other else me, per_chan)
                for h in halves:
                    for core in range(2):
                        to = zz * SLAB + x * 2 + core
                        sent = pl.ds(pl.multiple_of(((zz * HALVES + h) * 2 + core) * half, half), half)
                        src = partial.at[other, sent, at]
                        if direct:
                            start = pl.multiple_of(place * width + part * cols, LANES)
                            dst = out_hbm.at[chan, pl.ds(h * half, half), pl.ds(start, cols if other else width)]
                        else:
                            dst = out_hbm.at[chan, place, pl.ds(h * half, half), at]
                        remote = pltpu.make_async_remote_copy(
                            src_ref=src, dst_ref=dst, send_sem=part_send, recv_sem=part_recv,
                            device_id=(to, out_chan), device_id_type=MESH,
                        )
                        here = pltpu.make_async_copy(src, dst, part_recv)
                        stays = jnp.logical_and(to == me, owner_plane)
                        pl.when(stays)(here.start)
                        pl.when(jnp.logical_not(stays))(remote.start)

    def each(first, last, body):
        def run(g, _):
            body(g)
            return 0

        lax.fori_loop(first, last, run, 0)

    last = line - 1
    split = 2
    whole = tuple(range(HALVES))


    for h in range(HALVES):
        relay(1, h)
    compute(0, whole, 0, 0)
    compute(1, whole, 0, 0, True)
    each(split, last, lambda d: relay(d, 0))
    swapped(0).wait_recv()
    compute(1, whole, 1, 0, True)
    compute(0, whole, 1, 0)
    each(split, last, lambda d: relay(d, 1))
    compute(1, whole, 0, 0, False)
    each(split, last, lambda d: compute(d, whole, 0, 0))
    compute(1, whole, 1, 0, False)
    each(split, last, lambda d: compute(d, whole, 1, 0))
    for h in range(HALVES):
        relay(last, h)
    for part in range(1, parts):
        swapped(part).wait_recv()
        each(0, last, lambda d: compute(d, whole, 1, part))
    for h in range(HALVES):
        compute(last, (h,), 0, 0)
    for part in range(parts):
        compute(last, whole, 1, part)

    def drained(ref, sem):
        return pltpu.make_async_remote_copy(
            src_ref=ref, dst_ref=ref, send_sem=sem, recv_sem=sem, device_id=(sib, chan), device_id_type=MESH,
        )

    drained(out_hbm, part_recv).wait_recv()

    drained(ends_all.at[pl.ds(0, SLAB - 1)], end_send).wait_send()
    drained(starts_all.at[pl.ds(0, SLAB - 1)], start_send).wait_send()
    for hop in range(1, line):
        pl.when(z + hop < line)(carry_copy(hop).wait_send)
    for part in range(parts):
        swapped(part).wait_send()
    inner = jnp.logical_not(jnp.logical_or(taker, giver))
    pl.when(inner)(drained(gathered.at[pl.ds(0, (line + 1) * tok)], line_send).wait_send)
    pl.when(taker)(drained(gathered.at[pl.ds(0, tok)], line_send).wait_send)
    pl.when(giver)(drained(gathered.at[pl.ds(0, line * tok + tok // 2)], line_send).wait_send)
    for copy in near_copies:
        pl.when(giver)(copy.wait_send)
    drained(gathered.at[pl.ds(0, line * tok)], sib_send).wait_send()
    pl.when(owner_plane)(drained(partial.at[:, pl.ds(0, (2 * line - 1) * tok)], part_send).wait_send)
    pl.when(jnp.logical_not(owner_plane))(drained(partial, part_send).wait_send)


def solution(mesh):
    n, n_chan = mesh.shape["seq"], mesh.shape["chan"]
    assert n % (SLAB * n_chan) == 0 and n >= 4 * SLAB

    def body(gate_input, key_input, value_input, decay_rate, residue, skip_gain, out_weight):
        tok, chans = gate_input.shape
        modes = decay_rate.shape[0]
        width = out_weight.shape[1]
        line = n // SLAB
        quarter = modes * chans // (LANES * SLAB)
        rows = 2 * line * tok
        direct = width % LANES == 0
        hbm = pl.BlockSpec(memory_space=pltpu.HBM)
        dma = pltpu.SemaphoreType.DMA
        slab_states = pltpu.VMEM((SLAB, quarter, LANES), BF16)
        all_states = pltpu.VMEM((SLAB * quarter, LANES), BF16)
        per_chan = n // n_chan
        landing = (n_chan, tok, width * per_chan) if direct else (n_chan, per_chan, tok, width)
        landed = pl.pallas_call(
            functools.partial(kernel, n, n_chan),
            out_shape=jax.ShapeDtypeStruct(landing, BF16),
            in_specs=[hbm] * 7,
            out_specs=pl.BlockSpec(memory_space=pl.ANY),
            scratch_shapes=[
                pltpu.VMEM((tok, chans), BF16),
                pltpu.VMEM((tok, chans), BF16),
                pltpu.VMEM((tok, chans), BF16),
                pltpu.VMEM((modes, chans), F32),
                pltpu.VMEM((modes, chans), F32),
                pltpu.VMEM((1, chans), F32),
                pltpu.VMEM((chans, width), BF16),
                pltpu.VMEM((chans, width), BF16),
                dma((13,)), dma((column_parts(width),)), dma((column_parts(width),)),
                pltpu.VMEM((tok, chans), F32),
                pltpu.VMEM((tok, chans), F32),
                pltpu.VMEM((tok + SUB, LANES), F32),
                all_states, slab_states, pltpu.VMEM((line, quarter, LANES), BF16), pltpu.VMEM((quarter, LANES), BF16),
                slab_states, all_states,
                pltpu.VMEM((tok, chans), BF16), pltpu.VMEM((tok, chans), BF16), pltpu.VMEM((tok, chans), BF16), all_states,
                pltpu.VMEM((rows, chans), BF16),
                pltpu.VMEM((2, rows, width), BF16),
                pltpu.SemaphoreType.REGULAR, dma(()), dma(()), dma((line,)), dma((line,)), dma(()), dma((SLAB - 1,)),
                dma((3,)), dma((3,)), dma(()), dma((line * HALVES * SLAB,)), dma(()), dma((line * HALVES,)),
                dma(()), dma(()),
            ],
            compiler_params=pltpu.CompilerParams(
                collective_id=0, has_side_effects=True, vmem_limit_bytes=40 * 2**20
            ),
            cost_estimate=pl.CostEstimate(
                flops=2 * n * tok * chans * width, bytes_accessed=4 * tok * chans, transcendentals=0
            ),
        )(*[
            pltpu.with_memory_space_constraint(array, pltpu.HBM)
            for array in (
                gate_input, key_input, value_input, decay_rate, residue, skip_gain.reshape(1, chans), out_weight
            )
        ])
        mixed = landed[0].astype(F32)
        for j in range(1, n_chan):
            mixed = mixed + landed[j].astype(F32)
        mixed = mixed.astype(BF16)
        return mixed if direct else mixed.transpose(1, 0, 2).reshape(tok, width * per_chan)

    return jax.shard_map(
        body,
        mesh=mesh,
        in_specs=(
            P("seq", "chan"),
            P("seq", "chan"),
            P("seq", "chan"),
            P(None, "chan"),
            P(None, "chan"),
            P("chan"),
            P("chan", "seq"),
        ),
        out_specs=P("seq", "chan"),
        check_vma=False,
    )
```
